16 devices in a mesh: dp: 4 (over z, y), tp: 4 (over x, core).
Axes of the slice: x: 2, y: 2, z: 2, core: 2. Of those that a mesh axis runs over, the one named last changes fastest.
Arguments:
- tokens: int32 [384, 3], P('dp'), parts along dimension 0
- targets: int32 [384, 3], P('dp'), parts along dimension 0
- start_pos: int32 [384], P('dp'), parts along dimension 0
- embed_table: bfloat16 [262144, 1152], P('tp')
- layer_norms: float32 [2, 4, 1152], replicated
- w_q: bfloat16 [2, 1152, 4, 256], replicated
- w_k: bfloat16 [2, 1152, 1, 256], replicated
- w_v: bfloat16 [2, 1152, 1, 256], replicated
- qk_norms: float32 [2, 2, 256], replicated
- w_o: bfloat16 [2, 4, 256, 1152], replicated
- w_gate: bfloat16 [2, 1152, 6912], P(None, None, 'tp')
- w_up: bfloat16 [2, 1152, 6912], P(None, None, 'tp')
- w_down: bfloat16 [2, 6912, 1152], P(None, 'tp')
- norm_final: float32 [1152], replicated
- k_cache: bfloat16 [2, 384, 512, 1, 256], P(None, 'dp'), parts along dimension 1
- v_cache: bfloat16 [2, 384, 512, 1, 256], P(None, 'dp'), parts along dimension 1
Outputs:
- output 1: float32 [384, 3], P('dp'), parts along dimension 0
- output 2: float32 [384, 3], P('dp'), parts along dimension 0
- output 3: bfloat16 [2, 384, 512, 1, 256], P(None, 'dp'), parts along dimension 1
- output 4: bfloat16 [2, 384, 512, 1, 256], P(None, 'dp'), parts along dimension 1
There are 4 independent parts. The reference program is written for one: setup_inputs(seed, part) draws one part's arguments, and reference() takes and returns one part's arrays. A program takes and returns all parts, laid end to end along the dimension named above; an argument that names none is the same for every part.
All inputs are finite; a program needn't handle non-finite values.
Results may differ from the reference program's by a relative error of at most 0.0019836.
Values sent between devices are 32-bit elements.
A program may use at most 1.5 GiB of HBM per device.

```python
import jax
import jax.numpy as jnp
from jax import lax

VOCAB = 262144
D = 1152
HEADS = 4
KV_HEADS = 1
HEAD = 256
FF = 6912
WINDOW = 512
BATCH = 96
LAYERS = 2
STEPS = 3


def rms_norm(values, weight):
    values = values.astype(jnp.float32)
    mean_sq = jnp.mean(values * values, axis=-1, keepdims=True)
    return values * lax.rsqrt(mean_sq + 1e-6) * (1.0 + weight)


def apply_rope(vectors, positions):
    half_dim = vectors.shape[-1] // 2
    inv_freq = 10000.0 ** (-2.0 * jnp.arange(half_dim, dtype=jnp.float32) / vectors.shape[-1])
    angles = positions.astype(jnp.float32)[:, None] * inv_freq[None, :]
    cos_tab = jnp.cos(angles)[:, None, :]
    sin_tab = jnp.sin(angles)[:, None, :]
    first_half = vectors[..., :half_dim]
    second_half = vectors[..., half_dim:]
    return jnp.concatenate([first_half * cos_tab - second_half * sin_tab, second_half * cos_tab + first_half * sin_tab], axis=-1)


def setup_inputs(seed: int = 0, part: int = 0) -> dict:
    base_key = jax.random.key(seed)
    shared_keys = jax.random.split(base_key, 12)
    part_keys = jax.random.split(jax.random.fold_in(base_key, part), 8)
    row_ids = jnp.arange(BATCH)
    near_start = jax.random.randint(part_keys[0], (BATCH,), 0, 8)
    anywhere = jax.random.randint(part_keys[1], (BATCH,), 0, 2 * WINDOW)
    start_pos = jnp.where(row_ids % 2 == 0, near_start, anywhere)
    start_pos = start_pos.at[0].set(0).at[1].set(2 * WINDOW - 1)
    spread_ids = jnp.arange(8) * (VOCAB // 8)
    tokens = jax.random.randint(part_keys[2], (BATCH, STEPS), 0, VOCAB)
    tokens = tokens.at[:8, STEPS - 1].set(spread_ids + jax.random.randint(part_keys[3], (8,), 0, VOCAB // 8))
    tokens = tokens.at[0, 0].set(0).at[1, 0].set(VOCAB - 1)
    targets = jax.random.randint(part_keys[4], (BATCH, STEPS), 0, VOCAB)
    targets = targets.at[:8, STEPS - 1].set(spread_ids + jax.random.randint(part_keys[5], (8,), 0, VOCAB // 8))
    targets = targets.at[0, 1].set(0).at[1, 1].set(VOCAB - 1)
    norm_scale = jnp.array([0.5, 2.5, 0.5, 2.5], dtype=jnp.float32)
    norm_shift = jnp.array([0.0, 4.0, 0.0, 4.0], dtype=jnp.float32)
    embed_table = (jax.random.normal(shared_keys[0], (VOCAB, D), jnp.float32) * D ** -0.5).astype(jnp.bfloat16)
    layer_norms = jax.random.normal(shared_keys[1], (LAYERS, 4, D), jnp.float32) * norm_scale[None, :, None] + norm_shift[None, :, None]
    w_q = (jax.random.normal(shared_keys[2], (LAYERS, D, HEADS, HEAD), jnp.float32) * D ** -0.5).astype(jnp.bfloat16)
    w_k = (jax.random.normal(shared_keys[3], (LAYERS, D, KV_HEADS, HEAD), jnp.float32) * D ** -0.5).astype(jnp.bfloat16)
    w_v = (jax.random.normal(shared_keys[4], (LAYERS, D, KV_HEADS, HEAD), jnp.float32) * D ** -0.5).astype(jnp.bfloat16)
    qk_norms = 0.5 * jax.random.normal(shared_keys[5], (LAYERS, 2, HEAD), jnp.float32)
    w_o = (jax.random.normal(shared_keys[6], (LAYERS, HEADS, HEAD, D), jnp.float32) * (HEADS * HEAD) ** -0.5).astype(jnp.bfloat16)
    w_gate = (jax.random.normal(shared_keys[7], (LAYERS, D, FF), jnp.float32) * D ** -0.5).astype(jnp.bfloat16)
    w_up = (jax.random.normal(shared_keys[8], (LAYERS, D, FF), jnp.float32) * D ** -0.5).astype(jnp.bfloat16)
    w_down = (jax.random.normal(shared_keys[9], (LAYERS, FF, D), jnp.float32) * FF ** -0.5).astype(jnp.bfloat16)
    norm_final = 2.0 + 0.75 * jax.random.normal(shared_keys[10], (D,), jnp.float32)
    k_cache = jax.random.normal(part_keys[6], (LAYERS, BATCH, WINDOW, KV_HEADS, HEAD), jnp.float32).astype(jnp.bfloat16)
    v_cache = jax.random.normal(part_keys[7], (LAYERS, BATCH, WINDOW, KV_HEADS, HEAD), jnp.float32).astype(jnp.bfloat16)
    return {'tokens': tokens, 'targets': targets, 'start_pos': start_pos, 'embed_table': embed_table, 'layer_norms': layer_norms, 'w_q': w_q, 'w_k': w_k, 'w_v': w_v, 'qk_norms': qk_norms, 'w_o': w_o, 'w_gate': w_gate, 'w_up': w_up, 'w_down': w_down, 'norm_final': norm_final, 'k_cache': k_cache, 'v_cache': v_cache}


def reference(tokens, targets, start_pos, embed_table, layer_norms, w_q, w_k, w_v, qk_norms, w_o, w_gate, w_up, w_down, norm_final, k_cache, v_cache):
    batch_rows = tokens.shape[0]
    row_ids = jnp.arange(batch_rows)
    slot_ids = jnp.arange(WINDOW)
    group_size = HEADS // KV_HEADS
    normalizer = jnp.array(D ** 0.5, dtype=jnp.float32).astype(jnp.bfloat16).astype(jnp.float32)
    logprobs = []
    log_norms = []
    for step_idx in range(STEPS):
        positions = start_pos + step_idx
        slot_now = positions % WINDOW
        slot_valid = (positions[:, None] - (positions[:, None] - slot_ids[None, :]) % WINDOW) >= 0
        hidden = embed_table[tokens[:, step_idx]].astype(jnp.float32) * normalizer
        for layer_idx in range(LAYERS):
            normed = rms_norm(hidden, layer_norms[layer_idx, 0]).astype(jnp.bfloat16)
            query_all = jnp.dot(normed, w_q[layer_idx].reshape(D, HEADS * HEAD), preferred_element_type=jnp.float32).reshape(batch_rows, HEADS, HEAD)
            query_all = apply_rope(rms_norm(query_all, qk_norms[layer_idx, 0]), positions).astype(jnp.bfloat16)
            keys_new = jnp.dot(normed, w_k[layer_idx].reshape(D, KV_HEADS * HEAD), preferred_element_type=jnp.float32).reshape(batch_rows, KV_HEADS, HEAD)
            keys_new = apply_rope(rms_norm(keys_new, qk_norms[layer_idx, 1]), positions).astype(jnp.bfloat16)
            values_new = jnp.dot(normed, w_v[layer_idx].reshape(D, KV_HEADS * HEAD), preferred_element_type=jnp.float32).reshape(batch_rows, KV_HEADS, HEAD).astype(jnp.bfloat16)
            k_cache = k_cache.at[layer_idx, row_ids, slot_now].set(keys_new)
            v_cache = v_cache.at[layer_idx, row_ids, slot_now].set(values_new)
            grouped = query_all.reshape(batch_rows, KV_HEADS, group_size, HEAD).astype(jnp.float32)
            scores = jnp.einsum('bkge,bske->bkgs', grouped, k_cache[layer_idx].astype(jnp.float32)) * HEAD ** -0.5
            scores = jnp.where(slot_valid[:, None, None, :], scores, -1e30)
            attn_probs = jax.nn.softmax(scores, axis=-1).astype(jnp.bfloat16).astype(jnp.float32)
            attn_heads = jnp.einsum('bkgs,bske->bkge', attn_probs, v_cache[layer_idx].astype(jnp.float32)).astype(jnp.bfloat16)
            attn_out = jnp.dot(attn_heads.reshape(batch_rows, HEADS * HEAD), w_o[layer_idx].reshape(HEADS * HEAD, D), preferred_element_type=jnp.float32)
            hidden = hidden + rms_norm(attn_out, layer_norms[layer_idx, 1])
            mlp_in = rms_norm(hidden, layer_norms[layer_idx, 2]).astype(jnp.bfloat16)
            gate_proj = jnp.dot(mlp_in, w_gate[layer_idx], preferred_element_type=jnp.float32)
            up_proj = jnp.dot(mlp_in, w_up[layer_idx], preferred_element_type=jnp.float32)
            mlp_act = (jax.nn.gelu(gate_proj, approximate=True) * up_proj).astype(jnp.bfloat16)
            down_out = jnp.dot(mlp_act, w_down[layer_idx], preferred_element_type=jnp.float32)
            hidden = hidden + rms_norm(down_out, layer_norms[layer_idx, 3])
        final_normed = rms_norm(hidden, norm_final).astype(jnp.bfloat16)
        logits = lax.dot_general(final_normed, embed_table, (((1,), (1,)), ((), ())), preferred_element_type=jnp.float32)
        top_logit = jnp.max(logits, axis=-1)
        log_z = top_logit + jnp.log(jnp.sum(jnp.exp(logits - top_logit[:, None]), axis=-1))
        target_logit = jnp.take_along_axis(logits, targets[:, step_idx][:, None], axis=1)[:, 0]
        logprobs.append(target_logit - log_z)
        log_norms.append(log_z)
    return jnp.stack(logprobs, axis=1), jnp.stack(log_norms, axis=1), k_cache, v_cache
```

```python
import functools

import jax
import jax.numpy as jnp
import numpy as np
from jax import lax
from jax.experimental import pallas as pl
from jax.experimental.pallas import tpu as pltpu
from jax.sharding import PartitionSpec as P

EPSILON = 1e-6
ROPE_BASE = 10000.0
NEG = -1e30
MESH = pl.DeviceIdType.MESH
F32 = jnp.float32
BF16 = jnp.bfloat16
NT = (((1,), (1,)), ((), ()))
VMEM_LIMIT = 62 * 1024 * 1024


def rms(values, weight):
    mean_sq = jnp.mean(values * values, axis=-1, keepdims=True)
    return values * lax.rsqrt(mean_sq + EPSILON) * (1.0 + weight)


def vspec():
    return pl.BlockSpec(memory_space=pltpu.VMEM)


def aspec():
    return pl.BlockSpec(memory_space=pl.ANY)


def sspec():
    return pl.BlockSpec(memory_space=pltpu.SMEM)


def gather_kernel(rows, grp_ref, col_ref, table_ref, out_ref, xbuf, sem):
    def issue(i, carry):
        src = pl.multiple_of(grp_ref[i] * 8, 8)
        dst = pl.multiple_of(i * 8, 8)
        pltpu.make_async_copy(table_ref.at[pl.ds(src, 8), :], xbuf.at[pl.ds(dst, 8), :], sem).start()
        return carry

    lax.fori_loop(0, rows, issue, 0)
    pltpu.make_async_copy(table_ref.at[pl.ds(0, rows * 8), :], xbuf, sem).wait()
    for c in range(rows // 32):
        lanes = lax.broadcasted_iota(jnp.int32, (32, 256), 1)
        pick = jnp.where(lanes == col_ref[c * 32:(c + 1) * 32, :], 1.0, 0.0).astype(BF16)
        out_ref[c * 32:(c + 1) * 32, :] = jnp.dot(pick, xbuf[c * 256:(c + 1) * 256, :], preferred_element_type=F32)


def gather_rows(ids, table):
    rows = ids.shape[0]
    vocab_local, dim = table.shape
    here = (ids >= 0) & (ids < vocab_local)
    safe = jnp.clip(ids, 0, vocab_local - 1)
    col = jnp.where(here, (jnp.arange(rows) % 32) * 8 + safe % 8, -1)[:, None]
    return pl.pallas_call(
        functools.partial(gather_kernel, rows),
        out_shape=jax.ShapeDtypeStruct((rows, dim), F32),
        in_specs=[sspec(), vspec(), aspec()],
        out_specs=vspec(),
        scratch_shapes=[pltpu.VMEM((rows * 8, dim), BF16), pltpu.SemaphoreType.DMA],
        compiler_params=pltpu.CompilerParams(vmem_limit_bytes=24 * 1024 * 1024),
        name="token_rows",
    )(safe // 8, col, table)


def sum_kernel(rows, chunks, part_ref, out_ref, got1, half, got2, total, got3, s1, r1, s2, r2, s3, r3):
    dp = lax.axis_index("dp")
    tp = lax.axis_index("tp")
    core = lax.rem(tp, 2)
    mate = (dp, tp + 1 - 2 * core)
    across = (dp, lax.rem(tp + 2, 4))
    barrier = pltpu.get_barrier_semaphore()
    for peer in (mate, across):
        pl.semaphore_signal(barrier, inc=1, device_id=peer, device_id_type=MESH)
    pl.semaphore_wait(barrier, 2)
    hrows = rows // 2
    crows = hrows // chunks
    own = core * hrows
    other = (1 - core) * hrows

    def send(src, dst, ssem, rsem, peer):
        return pltpu.make_async_remote_copy(src_ref=src, dst_ref=dst, send_sem=ssem, recv_sem=rsem, device_id=peer, device_id_type=MESH)

    first, second, third = [], [], []
    for j in range(chunks):
        at = pl.multiple_of(other + j * crows, 8)
        first.append(send(part_ref.at[pl.ds(at, crows), :], got1.at[j], s1.at[j], r1.at[j], mate))
        first[-1].start()
    for j in range(chunks):
        first[j].wait_recv()
        at = pl.multiple_of(own + j * crows, 8)
        half[j] = part_ref[pl.ds(at, crows), :] + got1[j]
        second.append(send(half.at[j], got2.at[j], s2.at[j], r2.at[j], across))
        second[-1].start()
    for j in range(chunks):
        second[j].wait_recv()
        at = pl.multiple_of(own + j * crows, 8)
        value = half[j] + got2[j]
        total[j] = value
        out_ref[pl.ds(at, crows), :] = value
        third.append(send(total.at[j], got3.at[j], s3.at[j], r3.at[j], mate))
        third[-1].start()
    for j in range(chunks):
        third[j].wait_recv()
        at = pl.multiple_of(other + j * crows, 8)
        out_ref[pl.ds(at, crows), :] = got3[j]
    for j in range(chunks):
        first[j].wait_send()
        second[j].wait_send()
        third[j].wait_send()


def sum_tp(part, cid):
    rows, dim = part.shape
    chunks = 3
    buf = pltpu.VMEM((chunks, rows // 2 // chunks, dim), F32)
    sems = pltpu.SemaphoreType.DMA((chunks,))
    return pl.pallas_call(
        functools.partial(sum_kernel, rows, chunks),
        out_shape=jax.ShapeDtypeStruct((rows, dim), F32),
        in_specs=[vspec()],
        out_specs=vspec(),
        scratch_shapes=[buf] * 5 + [sems] * 6,
        compiler_params=pltpu.CompilerParams(collective_id=cid, has_side_effects=True, vmem_limit_bytes=24 * 1024 * 1024),
        name="sum_tp",
    )(part)


NB = 8
NBUF = 4


def layer_kernel(layer, batch, steps, normalizer, *refs):
    if layer == 0:
        (start_ref, startv_ref, cos_ref, sin_ref, ln_ref, qk_ref, ar_ref,
         wq_hbm, wk_hbm, wv_hbm, wo_hbm, wg_hbm, wu_hbm, wd_hbm, k_hbm, v_hbm,
         hid_ref, part_ref, ko_hbm, vo_hbm, *scratch) = refs
        prev_ref = None
    else:
        (start_ref, startv_ref, cos_ref, sin_ref, ln_ref, qk_ref, ar_ref, prev_ref,
         wq_hbm, wk_hbm, wv_hbm, wo_hbm, wg_hbm, wu_hbm, wd_hbm, k_hbm, v_hbm, _, _,
         hid_ref, part_ref, ko_hbm, vo_hbm, *scratch) = refs
    wq, wk, wv, wo, wg, wu, wd, kbuf, vbuf, qs, kn, vn, os, wsem, rsem, osem = scratch
    heads = 4
    nblk = batch // NB
    rows = batch * steps
    ln = lambda l, j: ln_ref[4 * l + j:4 * l + j + 1, :]

    weights = [(wq_hbm, wq), (wk_hbm, wk), (wv_hbm, wv), (wo_hbm, wo), (wg_hbm, wg), (wu_hbm, wu), (wd_hbm, wd)]
    wcopies = [pltpu.make_async_copy(src.at[layer], dst, wsem.at[n]) for n, (src, dst) in enumerate(weights)]

    def reads(i, slot):
        at = pl.ds(pl.multiple_of(i * NB, NB), NB)
        return (pltpu.make_async_copy(k_hbm.at[layer, at], kbuf.at[slot], rsem.at[0, slot]),
                pltpu.make_async_copy(v_hbm.at[layer, at], vbuf.at[slot], rsem.at[1, slot]))

    def writes(i, slot):
        at = pl.ds(pl.multiple_of(i * NB, NB), NB)
        return (pltpu.make_async_copy(kbuf.at[slot], ko_hbm.at[layer, at], osem.at[0, slot]),
                pltpu.make_async_copy(vbuf.at[slot], vo_hbm.at[layer, at], osem.at[1, slot]))

    for c in wcopies[:3]:
        c.start()
    for i in range(2):
        for c in reads(i, i):
            c.start()
    for c in wcopies[3:]:
        c.start()

    if layer == 0:
        hid = ar_ref[...] * normalizer
    else:
        hid = prev_ref[...] + rms(ar_ref[...], ln(layer - 1, 3))
    hid_ref[...] = hid
    act = rms(hid, ln(layer, 0)).astype(BF16)
    qs[...] = jnp.zeros_like(qs)
    kn[...] = jnp.zeros_like(kn)
    vn[...] = jnp.zeros_like(vn)
    for c in wcopies[:3]:
        c.wait()

    def put(dst, j, values, lane):
        for t in range(steps):
            dst[lane, pl.ds(t * j[0] + j[1], batch, stride=16), :] = values[t * batch:(t + 1) * batch, :]

    def wide(ref, at):
        return jnp.concatenate([ref[0, at, :], ref[1, at, :]], axis=1)

    def roped(x, weight):
        x = rms(x, weight)
        a, b = x[:, :128], x[:, 128:]
        c, s = cos_ref[...], sin_ref[...]
        return a * c - b * s, b * c + a * s

    for h in range(heads):
        q = jnp.dot(act, wq[:, h * 256:(h + 1) * 256], preferred_element_type=F32)
        lo, hi = roped(q, qk_ref[2 * layer:2 * layer + 1, :])
        put(qs, (heads, h), lo, 0)
        put(qs, (heads, h), hi, 1)
    k = jnp.dot(act, wk[...], preferred_element_type=F32)
    lo, hi = roped(k, qk_ref[2 * layer + 1:2 * layer + 2, :])
    put(kn, (1, 0), lo, 0)
    put(kn, (1, 0), hi, 1)
    v = jnp.dot(act, wv[...], preferred_element_type=F32)
    put(vn, (1, 0), v[:, :128], 0)
    put(vn, (1, 0), v[:, 128:], 1)

    scale = 256 ** -0.5
    m_rows = NB * 16

    def block(i, carry):
        slot = lax.rem(i, NBUF)
        for c in reads(i, slot):
            c.wait()

        @pl.when(i >= 1)
        def _():
            for c in writes(i - 1, lax.rem(i + NBUF - 1, NBUF)):
                c.start()

        @pl.when(i >= 2)
        def _():
            for c in writes(i - 2, lax.rem(i + NBUF - 2, NBUF)):
                c.wait()

        @pl.when(i + 2 < nblk)
        def _():
            for c in reads(i + 2, lax.rem(i + 2, NBUF)):
                c.start()

        r0 = pl.multiple_of(i * m_rows, m_rows)
        at = pl.ds(r0, m_rows)
        qb = wide(qs, at).astype(BF16)
        knf = wide(kn, at)
        vnf = wide(vn, at)
        start = startv_ref[at, :]
        row = lax.broadcasted_iota(jnp.int32, (m_rows, 128), 0)
        lane = lax.broadcasted_iota(jnp.int32, (m_rows, 128), 1)
        t = lax.shift_right_logical(row & 15, 2)
        old = jnp.concatenate([lax.dot_general(qb[16 * j:16 * j + 16, :], kbuf[slot, j], NT, preferred_element_type=F32) for j in range(NB)], axis=0) * scale
        new = lax.dot_general(qb, knf.astype(BF16), NT, preferred_element_type=F32) * scale
        cols = []
        for g in range(4):
            s = lane + 128 * g
            ok = (s <= start + t) & (((s - start) & 511) > t)
            cols.append(jnp.where(ok, old[:, 128 * g:128 * (g + 1)], NEG))
        ok = (lax.shift_right_logical(row, 4) == lax.shift_right_logical(lane, 4)) & ((lane & 15) <= t)
        cols.append(jnp.where(ok, new, NEG))
        top = jnp.maximum(jnp.maximum(jnp.maximum(cols[0], cols[1]), jnp.maximum(cols[2], cols[3])), cols[4])
        top = jnp.max(top, axis=-1, keepdims=True)
        exps = [jnp.exp(c - top) for c in cols]
        tot = jnp.sum((exps[0] + exps[1]) + (exps[2] + exps[3]) + exps[4], axis=-1, keepdims=True)
        inv = 1.0 / tot
        pold = jnp.concatenate([(e * inv).astype(BF16) for e in exps[:4]], axis=1)
        pnew = (exps[4] * inv).astype(BF16)
        out = jnp.dot(pnew, vnf.astype(BF16), preferred_element_type=F32)
        out = out + jnp.concatenate([jnp.dot(pold[16 * j:16 * j + 16, :], vbuf[slot, j], preferred_element_type=F32) for j in range(NB)], axis=0)
        os[0, at, :] = out[:, :128]
        os[1, at, :] = out[:, 128:]

        sub = lax.broadcasted_iota(jnp.int32, (16, 256), 0)
        for half in range(2):
            pending = []
            for j in range(half * NB // 2, (half + 1) * NB // 2):
                st = start_ref[i * NB + j]
                for w in (st & 511, (st + 2) & 511):
                    w = pl.multiple_of(lax.shift_left(lax.shift_right_logical(w, 4), 4), 16)
                    dist = (sub + w - st) & 511
                    for buf, fresh in ((kbuf, knf), (vbuf, vnf)):
                        value = buf[slot, j, pl.ds(w, 16), :].astype(F32)
                        for tt in range(steps):
                            value = jnp.where(dist == tt, fresh[16 * j + tt:16 * j + tt + 1, :], value)
                        pending.append((buf, j, w, value.astype(BF16)))
            for buf, j, w, value in pending:
                buf[slot, j, pl.ds(w, 16), :] = value
        return carry

    lax.fori_loop(0, nblk, block, 0)
    for c in writes(nblk - 1, (nblk - 1) % NBUF):
        c.start()

    wcopies[3].wait()
    attn = None
    for h in range(heads):
        parts = []
        for t in range(steps):
            parts.append(jnp.concatenate([os[g, pl.ds(t * heads + h, batch, stride=16), :] for g in range(2)], axis=1))
        x = jnp.concatenate(parts, axis=0).astype(BF16)
        y = jnp.dot(x, wo[h * 256:(h + 1) * 256, :], preferred_element_type=F32)
        attn = y if attn is None else attn + y
    hid = hid_ref[...] + rms(attn, ln(layer, 1))
    hid_ref[...] = hid
    act = rms(hid, ln(layer, 2)).astype(BF16)
    for c in wcopies[4:]:
        c.wait()
    width = wg.shape[0]
    for at in range(0, width, 512):
        n = min(512, width - at)
        gate = lax.dot_general(act, wg[at:at + n, :], NT, preferred_element_type=F32)
        up = lax.dot_general(act, wu[at:at + n, :], NT, preferred_element_type=F32)
        inner = (jax.nn.gelu(gate, approximate=True) * up).astype(BF16)
        down = jnp.dot(inner, wd[at:at + n, :], preferred_element_type=F32)
        if at == 0:
            part_ref[...] = down
        else:
            part_ref[...] += down
    for i in (nblk - 2, nblk - 1):
        for c in writes(i, i % NBUF):
            c.wait()


def run_layer(layer, small, ar, prev, weights, caches, outs):
    batch = small[0].shape[0]
    rows, dim = ar.shape
    steps = rows // batch
    normalizer = float(np.float32(dim ** 0.5).astype(BF16))
    kc, vc = caches
    width = weights[4].shape[1]
    ins = list(small) + [ar] + ([] if prev is None else [prev]) + list(weights) + [kc, vc]
    specs = [sspec()] + [vspec()] * (len(small) - 1) + [vspec()] * (1 if prev is None else 2) + [aspec()] * 9
    alias = {}
    if outs is not None:
        alias = {len(ins): 2, len(ins) + 1: 3}
        ins += list(outs)
        specs += [aspec()] * 2
    scratch = [
        pltpu.VMEM((dim, 1024), BF16), pltpu.VMEM((dim, 256), BF16), pltpu.VMEM((dim, 256), BF16),
        pltpu.VMEM((1024, dim), BF16), pltpu.VMEM((width, dim), BF16), pltpu.VMEM((width, dim), BF16), pltpu.VMEM((width, dim), BF16),
        pltpu.VMEM((NBUF, NB, 512, 256), BF16), pltpu.VMEM((NBUF, NB, 512, 256), BF16),
        pltpu.VMEM((2, batch * 16, 128), F32), pltpu.VMEM((2, batch * 16, 128), F32), pltpu.VMEM((2, batch * 16, 128), F32), pltpu.VMEM((2, batch * 16, 128), F32),
        pltpu.SemaphoreType.DMA((7,)), pltpu.SemaphoreType.DMA((2, NBUF)), pltpu.SemaphoreType.DMA((2, NBUF)),
    ]
    return pl.pallas_call(
        functools.partial(layer_kernel, layer, batch, steps, normalizer),
        out_shape=[jax.ShapeDtypeStruct((rows, dim), F32), jax.ShapeDtypeStruct((rows, dim), F32),
                   jax.ShapeDtypeStruct(kc.shape, kc.dtype), jax.ShapeDtypeStruct(vc.shape, vc.dtype)],
        in_specs=specs,
        out_specs=[vspec(), vspec(), aspec(), aspec()],
        scratch_shapes=scratch,
        input_output_aliases=alias,
        compiler_params=pltpu.CompilerParams(vmem_limit_bytes=VMEM_LIMIT),
        name=f"layer{layer}",
    )(*ins)


TV = 1024
EBUF = 8


def scores_kernel(nblk, ar_ref, prev_ref, ln_ref, nf_ref, tgt_ref, e_hbm, out_ref, f_ref, ebuf, za, zb, m_ref, s_ref, t_ref, sem):
    rows, dim = f_ref.shape

    def fetch(i, slot):
        return pltpu.make_async_copy(e_hbm.at[pl.ds(pl.multiple_of(i * TV, TV), TV), :], ebuf.at[slot], sem.at[slot])

    for i in range(EBUF - 2):
        fetch(i, i).start()
    hid = prev_ref[...] + rms(ar_ref[...], ln_ref[7:8, :])
    f_ref[...] = rms(hid, nf_ref[...]).astype(BF16)
    m_ref[...] = jnp.full_like(m_ref, -jnp.inf)
    s_ref[...] = jnp.zeros_like(s_ref)
    t_ref[...] = jnp.zeros_like(t_ref)

    def dots(slot, z):
        for c in range(TV // 256):
            z[:, c * 256:(c + 1) * 256] = lax.dot_general(f_ref[...], ebuf[slot, c * 256:(c + 1) * 256, :], NT, preferred_element_type=F32)

    def fold(i, z):
        for r in range(rows // 8):
            sl = slice(r * 8, (r + 1) * 8)
            vals = [z[sl, g * 128:(g + 1) * 128] for g in range(TV // 128)]
            top = m_ref[sl, :]
            tops = list(vals)
            while len(tops) > 1:
                tops = [jnp.maximum(tops[n], tops[n + 1]) for n in range(0, len(tops), 2)]
            new = jnp.maximum(top, tops[0])
            m_ref[sl, :] = new
            exps = [jnp.exp(v - new) for v in vals]
            while len(exps) > 1:
                exps = [exps[n] + exps[n + 1] for n in range(0, len(exps), 2)]
            s_ref[sl, :] = s_ref[sl, :] * jnp.exp(top - new) + exps[0]
            want = tgt_ref[sl, :]
            hit = t_ref[sl, :]
            for g, v in enumerate(vals):
                hit = jnp.where(want == i * TV + g * 128, v, hit)
            t_ref[sl, :] = hit

    def prep(i, slot):
        fetch(i, slot).wait()

    def more(i):
        @pl.when(i < nblk)
        def _():
            fetch(i, lax.rem(i, EBUF)).start()

    fetch(0, 0).wait()
    more(EBUF - 2)
    dots(0, za)

    def pair(n, carry):
        a = 2 * n + 1
        b = a + 1
        prep(a, lax.rem(a, EBUF))
        prep(b, lax.rem(b, EBUF))
        more(a + EBUF - 2)
        more(b + EBUF - 2)
        dots(lax.rem(a, EBUF), zb)
        fold(a - 1, za)
        dots(lax.rem(b, EBUF), za)
        fold(a, zb)
        return carry

    lax.fori_loop(0, (nblk - 2) // 2, pair, 0)
    last = nblk - 1
    prep(last, last % EBUF)
    dots(last % EBUF, zb)
    fold(last - 1, za)
    fold(last, zb)

    m = m_ref[...]
    top = jnp.max(m, axis=-1, keepdims=True)
    tot = jnp.sum(s_ref[...] * jnp.exp(m - top), axis=-1, keepdims=True)
    tgt = jnp.sum(t_ref[...], axis=-1, keepdims=True)
    lane = lax.broadcasted_iota(jnp.int32, (rows, 128), 1)
    pack = jnp.where(lane == 0, top, jnp.where(lane == 1, tot, jnp.where(lane == 2, tgt, 0.0)))
    pad = out_ref.shape[1] - rows
    pack = jnp.concatenate([pack, jnp.zeros((pad, 128), F32)], axis=0)
    out_ref[...] = jnp.transpose(pack)[:8, :]


def table_scores(ar, prev, ln, nf, tgt, table):
    rows, dim = ar.shape
    nblk = table.shape[0] // TV
    lanes = -(-rows // 128) * 128
    return pl.pallas_call(
        functools.partial(scores_kernel, nblk),
        out_shape=jax.ShapeDtypeStruct((8, lanes), F32),
        in_specs=[vspec()] * 5 + [aspec()],
        out_specs=vspec(),
        scratch_shapes=[
            pltpu.VMEM((rows, dim), BF16), pltpu.VMEM((EBUF, TV, dim), BF16),
            pltpu.VMEM((rows, TV), F32), pltpu.VMEM((rows, TV), F32),
            pltpu.VMEM((rows, 128), F32), pltpu.VMEM((rows, 128), F32), pltpu.VMEM((rows, 128), F32),
            pltpu.SemaphoreType.DMA((EBUF,)),
        ],
        compiler_params=pltpu.CompilerParams(vmem_limit_bytes=VMEM_LIMIT),
        name="table_scores",
    )(ar, prev, ln, nf, tgt, table)


def combine_kernel(x_ref, out_ref, got, ssem, rsem):
    dp = lax.axis_index("dp")
    tp = lax.axis_index("tp")
    barrier = pltpu.get_barrier_semaphore()
    for d in range(1, 4):
        pl.semaphore_signal(barrier, inc=1, device_id=(dp, lax.rem(tp + d, 4)), device_id_type=MESH)
    pl.semaphore_wait(barrier, 3)
    sends = []
    for d in range(1, 4):
        sends.append(pltpu.make_async_remote_copy(src_ref=x_ref, dst_ref=got.at[d - 1], send_sem=ssem.at[d - 1], recv_sem=rsem.at[d - 1],
                                                  device_id=(dp, lax.rem(tp + d, 4)), device_id_type=MESH))
        sends[-1].start()
    for s in sends:
        s.wait()
    mine = x_ref[...]
    vals = [mine] + [got[d] for d in range(3)]
    ordered = []
    for dev in range(4):
        v = mine
        for d in range(1, 4):
            v = jnp.where(lax.rem(tp + 4 - d, 4) == dev, vals[d], v)
        ordered.append(v)
    top = jnp.maximum(jnp.maximum(ordered[0][0:1], ordered[1][0:1]), jnp.maximum(ordered[2][0:1], ordered[3][0:1]))
    tot = 0.0
    tgt = 0.0
    for v in ordered:
        tot = tot + v[1:2] * jnp.exp(v[0:1] - top)
        tgt = tgt + v[2:3]
    log_z = top + jnp.log(tot)
    lanes = out_ref.shape[1]
    row = lax.broadcasted_iota(jnp.int32, (8, lanes), 0)
    out_ref[...] = jnp.where(row == 0, tgt - log_z, log_z)


def combine(x, cid):
    return pl.pallas_call(
        combine_kernel,
        out_shape=jax.ShapeDtypeStruct(x.shape, F32),
        in_specs=[vspec()],
        out_specs=vspec(),
        scratch_shapes=[pltpu.VMEM((3,) + x.shape, F32), pltpu.SemaphoreType.DMA((3,)), pltpu.SemaphoreType.DMA((3,))],
        compiler_params=pltpu.CompilerParams(collective_id=cid, has_side_effects=True),
        name="combine_tp",
    )(x)


def solution(mesh):
    arg_specs = (P('dp', None), P('dp', None), P('dp'), P('tp', None), P(), P(), P(), P(), P(), P(), P(None, None, 'tp'), P(None, None, 'tp'), P(None, 'tp', None), P(), P(None, 'dp'), P(None, 'dp'))
    result_specs = (P('dp', None), P('dp', None), P(None, 'dp'), P(None, 'dp'))

    def decode_local(tokens, targets, start_pos, embed_table, layer_norms, w_q, w_k, w_v, qk_norms, w_o, w_gate, w_up, w_down, norm_final, k_cache, v_cache):
        batch, steps = tokens.shape
        layers, dim, heads, head_dim = w_q.shape
        window = k_cache.shape[2]
        vocab_local = embed_table.shape[0]
        rows = batch * steps
        vocab_start = lax.axis_index('tp') * vocab_local
        positions = (start_pos[None, :] + jnp.arange(steps)[:, None]).reshape(rows)
        inv_freq = ROPE_BASE ** (-2.0 * jnp.arange(head_dim // 2, dtype=F32) / head_dim)
        angles = positions.astype(F32)[:, None] * inv_freq[None, :]
        startv = jnp.broadcast_to(start_pos[:, None, None], (batch, 16, 128)).reshape(batch * 16, 128)
        ln = layer_norms.reshape(layers * 4, dim)
        small = (start_pos, startv, jnp.cos(angles), jnp.sin(angles), ln, qk_norms.reshape(layers * 2, head_dim))
        weights = (w_q.reshape(layers, dim, heads * head_dim), w_k.reshape(layers, dim, head_dim), w_v.reshape(layers, dim, head_dim),
                   w_o.reshape(layers, heads * head_dim, dim), jnp.swapaxes(w_gate, 1, 2), jnp.swapaxes(w_up, 1, 2), w_down)
        caches = (k_cache.reshape(layers, batch, window, head_dim), v_cache.reshape(layers, batch, window, head_dim))
        ar = sum_tp(gather_rows(tokens.T.reshape(rows) - vocab_start, embed_table), 0)
        hid, outs = None, None
        for layer in range(layers):
            hid, part, kc, vc = run_layer(layer, small, ar, hid, weights, caches, outs)
            outs = (kc, vc)
            ar = sum_tp(part, 1 + layer)
        tgt = (targets.T.reshape(rows) - vocab_start)[:, None] - jnp.arange(128)[None, :]
        stats = table_scores(ar, hid, ln, norm_final.reshape(1, dim), tgt, embed_table)
        res = combine(stats, 1 + layers)
        logprob = res[0, :rows].reshape(steps, batch).T
        log_z = res[1, :rows].reshape(steps, batch).T
        return logprob, log_z, outs[0].reshape(k_cache.shape), outs[1].reshape(v_cache.shape)

    return jax.shard_map(decode_local, mesh=mesh, in_specs=arg_specs, out_specs=result_specs, check_vma=False)
```

```python
import functools

import jax
import jax.numpy as jnp
import numpy as np
from jax import lax
from jax.experimental import pallas as pl
from jax.experimental.pallas import tpu as pltpu
from jax.sharding import PartitionSpec as P

EPSILON = 1e-6
ROPE_BASE = 10000.0
NEG = -1e30
MESH = pl.DeviceIdType.MESH
F32 = jnp.float32
BF16 = jnp.bfloat16
NT = (((1,), (1,)), ((), ()))


def rms(values, weight):
    mean_sq = jnp.mean(values * values, axis=-1, keepdims=True)
    return values * lax.rsqrt(mean_sq + EPSILON) * (1.0 + weight)


def vspec():
    return pl.BlockSpec(memory_space=pltpu.VMEM)


def aspec():
    return pl.BlockSpec(memory_space=pl.ANY)


def sspec():
    return pl.BlockSpec(memory_space=pltpu.SMEM)


def gather_kernel(rows, grp_ref, col_ref, table_ref, out_ref, xbuf, sem):
    def issue(i, carry):
        src = pl.multiple_of(grp_ref[i] * 8, 8)
        dst = pl.multiple_of(i * 8, 8)
        pltpu.make_async_copy(table_ref.at[pl.ds(src, 8), :], xbuf.at[pl.ds(dst, 8), :], sem).start()
        return carry

    lax.fori_loop(0, rows, issue, 0, unroll=8)
    pltpu.make_async_copy(table_ref.at[pl.ds(0, rows * 8), :], xbuf, sem).wait()
    for c in range(rows // 32):
        lanes = lax.broadcasted_iota(jnp.int32, (32, 256), 1)
        pick = jnp.where(lanes == col_ref[c * 32:(c + 1) * 32, :], 1.0, 0.0).astype(BF16)
        out_ref[c * 32:(c + 1) * 32, :] = jnp.dot(pick, xbuf[c * 256:(c + 1) * 256, :], preferred_element_type=F32)


def gather_rows(ids, table):
    rows = ids.shape[0]
    vocab_local, dim = table.shape
    here = (ids >= 0) & (ids < vocab_local)
    safe = jnp.clip(ids, 0, vocab_local - 1)
    col = jnp.where(here, (jnp.arange(rows) % 32) * 8 + safe % 8, -1)[:, None]
    return pl.pallas_call(
        functools.partial(gather_kernel, rows),
        out_shape=jax.ShapeDtypeStruct((rows, dim), F32),
        in_specs=[sspec(), vspec(), aspec()],
        out_specs=vspec(),
        scratch_shapes=[pltpu.VMEM((rows * 8, dim), BF16), pltpu.SemaphoreType.DMA],
        compiler_params=pltpu.CompilerParams(vmem_limit_bytes=24 * 1024 * 1024),
        name="token_rows",
    )(safe // 8, col, table)


LANES = 128
HEAD = 2 * LANES
TILE = 16
WINDOW = 512
MIB = 1024 * 1024


def mate_of():
    tp = lax.axis_index("tp")
    core = lax.rem(tp, 2)
    return core, (lax.axis_index("dp"), tp + 1 - 2 * core)


def meet(mate):
    barrier = pltpu.get_barrier_semaphore()
    pl.semaphore_signal(barrier, inc=1, device_id=mate, device_id_type=MESH)
    pl.semaphore_wait(barrier, 1)


def send(src, dst, ssem, rsem, peer):
    return pltpu.make_async_remote_copy(src_ref=src, dst_ref=dst, send_sem=ssem, recv_sem=rsem, device_id=peer, device_id_type=MESH)


def part_rows(which, ref):
    hrows = ref.shape[0] // 2
    return pl.ds(pl.multiple_of(which * hrows, 8), hrows)


def mate_sum(part_ref, out_ref, got, ssem, rsem, core, mate):
    swap = send(part_ref.at[part_rows(1 - core, part_ref), :], got, ssem, rsem, mate)
    swap.start()
    swap.wait()
    out_ref[...] = part_ref[part_rows(core, part_ref), :] + got[...]


def pair_sum_kernel(part_ref, out_ref, got, ssem, rsem):
    core, mate = mate_of()
    meet(mate)
    mate_sum(part_ref, out_ref, got, ssem, rsem, core, mate)


def pair_share_kernel(a_ref, b_ref, out_ref, total, got, ssem, rsem):
    core, mate = mate_of()
    total[...] = a_ref[...] + b_ref[...]
    meet(mate)
    swap = send(total, got, ssem, rsem, mate)
    swap.start()
    out_ref[part_rows(core, out_ref), :] = total[...]
    swap.wait()
    out_ref[part_rows(1 - core, out_ref), :] = got[...]


def pair_call(kernel, out_rows, ins, scratch, cid, name):
    dim = ins[0].shape[1]
    return pl.pallas_call(
        kernel,
        out_shape=jax.ShapeDtypeStruct((out_rows, dim), F32),
        in_specs=[vspec()] * len(ins),
        out_specs=vspec(),
        scratch_shapes=[pltpu.VMEM(shape, F32) for shape in scratch] + [pltpu.SemaphoreType.DMA] * 2,
        compiler_params=pltpu.CompilerParams(collective_id=cid, has_side_effects=True, vmem_limit_bytes=12 * MIB),
        name=name,
    )(*ins)


def pair_sum(part, cid):
    rows, dim = part.shape
    return pair_call(pair_sum_kernel, rows // 2, [part], [(rows // 2, dim)], cid, "pair_sum")


def share(half, cid):
    far = lax.ppermute(half, 'tp', [(n, (n + 2) % 4) for n in range(4)])
    return pair_call(pair_share_kernel, half.shape[0] * 2, [half, far], [half.shape] * 2, cid, "pair_share")


NB = 8
NBUF = 4


class Stream:
    def __init__(self, layer, base, sources, targets, bufs, rsem, osem):
        self.layer, self.base = layer, base
        self.sources, self.targets, self.bufs, self.rsem, self.osem = sources, targets, bufs, rsem, osem

    def rows(self, i):
        return pl.ds(pl.multiple_of(self.base + i * NB, NB), NB)

    def reads(self, i, slot):
        return [pltpu.make_async_copy(src.at[self.layer, self.rows(i)], buf.at[slot], self.rsem.at[n, slot])
                for n, (src, buf) in enumerate(zip(self.sources, self.bufs))]

    def writes(self, i, slot):
        return [pltpu.make_async_copy(buf.at[slot], dst.at[self.layer, self.rows(i)], self.osem.at[n, slot])
                for n, (dst, buf) in enumerate(zip(self.targets, self.bufs))]

    def begin(self):
        for i in range(2):
            for c in self.reads(i, i):
                c.start()

    def run(self, nblk, body):
        def block(i, carry):
            slot = lax.rem(i, NBUF)
            for c in self.reads(i, slot):
                c.wait()

            @pl.when(i >= 1)
            def _():
                for c in self.writes(i - 1, lax.rem(i + NBUF - 1, NBUF)):
                    c.start()

            @pl.when(i >= 2)
            def _():
                for c in self.writes(i - 2, lax.rem(i + NBUF - 2, NBUF)):
                    c.wait()

            @pl.when(i + 2 < nblk)
            def _():
                for c in self.reads(i + 2, lax.rem(i + 2, NBUF)):
                    c.start()

            body(i, slot)
            return carry

        lax.fori_loop(0, nblk, block, 0)
        for c in self.writes(nblk - 1, (nblk - 1) % NBUF):
            c.start()

    def end(self, nblk):
        for i in (nblk - 2, nblk - 1):
            for c in self.writes(i, i % NBUF):
                c.wait()

    def change(self, i, slot, start_ref, fresh, steps):
        sub = lax.broadcasted_iota(jnp.int32, (TILE, HEAD), 0)
        for first in (0, NB // 2):
            pending = []
            for j in range(first, first + NB // 2):
                st = start_ref[self.base + i * NB + j]
                for s in (st & (WINDOW - 1), (st + steps - 1) & (WINDOW - 1)):
                    at = pl.multiple_of(s - (s & (TILE - 1)), TILE)
                    dist = (sub + at - st) & (WINDOW - 1)
                    for buf, new in zip(self.bufs, fresh):
                        value = buf[slot, j, pl.ds(at, TILE), :].astype(F32)
                        for t in range(steps):
                            value = jnp.where(dist == t, new[TILE * j + t:TILE * j + t + 1, :], value)
                        pending.append((buf, j, at, value.astype(BF16)))
            for buf, j, at, value in pending:
                buf[slot, j, pl.ds(at, TILE), :] = value


def stream_scratch():
    buf = pltpu.VMEM((NBUF, NB, WINDOW, HEAD), BF16)
    sem = pltpu.SemaphoreType.DMA((2, NBUF))
    return [buf, buf, sem, sem]


def cache_shapes(caches):
    return [jax.ShapeDtypeStruct(c.shape, c.dtype) for c in caches]


def wide(ref, n, at):
    return jnp.concatenate([ref[n, at, :], ref[n + 1, at, :]], axis=1)


def tiles(i):
    return pl.ds(pl.multiple_of(i * NB * TILE, NB * TILE), NB * TILE)


def carry_kernel(layer, steps, core_ref, start_ref, fresh, k_hbm, v_hbm, _k, _v, ko_hbm, vo_hbm, kbuf, vbuf, rsem, osem):
    half = fresh.shape[1] // TILE
    nblk = half // NB
    stream = Stream(layer, (1 - core_ref[0]) * half, (k_hbm, v_hbm), (ko_hbm, vo_hbm), (kbuf, vbuf), rsem, osem)
    stream.begin()
    stream.run(nblk, lambda i, slot: stream.change(i, slot, start_ref, (wide(fresh, 0, tiles(i)), wide(fresh, 2, tiles(i))), steps))
    stream.end(nblk)


def carry_other(layer, steps, core, start, fresh, caches, outs):
    return pl.pallas_call(
        functools.partial(carry_kernel, layer, steps),
        out_shape=cache_shapes(caches),
        in_specs=[sspec(), sspec(), vspec()] + [aspec()] * 4,
        out_specs=[aspec()] * 2,
        scratch_shapes=stream_scratch(),
        input_output_aliases={5: 0, 6: 1},
        compiler_params=pltpu.CompilerParams(vmem_limit_bytes=24 * MIB),
        cost_estimate=pl.CostEstimate(flops=10 ** 10, bytes_accessed=48 * MIB, transcendentals=0),
        name=f"carry{layer}",
    )(core, start, fresh, *caches, *outs)


def feed_kernel(layer, heads_ref, hid_ref, ln_ref, wo_hbm, wg_hbm, wu_hbm, wd_hbm,
                hid_out, half_ref, wo, wg, wu, wd, both, part, got, wsem, hsend, hrecv, ssem, rsem):
    core, mate = mate_of()
    weights = [(wo_hbm, wo), (wg_hbm, wg), (wu_hbm, wu), (wd_hbm, wd)]
    wcopies = [pltpu.make_async_copy(src.at[layer], dst, wsem.at[n]) for n, (src, dst) in enumerate(weights)]
    for c in wcopies:
        c.start()
    meet(mate)
    swap = send(heads_ref, both.at[core], hsend, hrecv, mate)
    swap.start()
    both[core] = heads_ref[...]
    ln = lambda j: ln_ref[4 * layer + j:4 * layer + j + 1, :]
    wcopies[0].wait()
    swap.wait_recv()
    x = jnp.concatenate([both[0], both[1]], axis=0).astype(BF16)
    hid = hid_ref[...] + rms(jnp.dot(x, wo[...], preferred_element_type=F32), ln(1))
    hid_out[...] = hid
    act = rms(hid, ln(2)).astype(BF16)
    for c in wcopies[1:]:
        c.wait()
    width = wg.shape[0]
    for at in range(0, width, WINDOW):
        cut = slice(at, min(at + WINDOW, width))
        gate = lax.dot_general(act, wg[cut, :], NT, preferred_element_type=F32)
        up = lax.dot_general(act, wu[cut, :], NT, preferred_element_type=F32)
        inner = (jax.nn.gelu(gate, approximate=True) * up).astype(BF16)
        down = jnp.dot(inner, wd[cut, :], preferred_element_type=F32)
        if at == 0:
            part[...] = down
        else:
            part[...] += down
    swap.wait_send()
    mate_sum(part, half_ref, got, ssem, rsem, core, mate)


def feed(layer, heads, hid, ln, weights, cid):
    rows, dim = hid.shape
    width = weights[1].shape[1]
    own, inner = heads.shape
    return pl.pallas_call(
        functools.partial(feed_kernel, layer),
        out_shape=[jax.ShapeDtypeStruct((rows, dim), F32), jax.ShapeDtypeStruct((own, dim), F32)],
        in_specs=[vspec()] * 3 + [aspec()] * 4,
        out_specs=[vspec()] * 2,
        scratch_shapes=[pltpu.VMEM((inner, dim), BF16)] + [pltpu.VMEM((width, dim), BF16)] * 3 + [
            pltpu.VMEM((2, own, inner), F32), pltpu.VMEM((rows, dim), F32), pltpu.VMEM((own, dim), F32),
            pltpu.SemaphoreType.DMA((4,))] + [pltpu.SemaphoreType.DMA] * 4,
        compiler_params=pltpu.CompilerParams(collective_id=cid, has_side_effects=True, vmem_limit_bytes=40 * MIB),
        name=f"feed{layer}",
    )(heads, hid, ln, *weights)


def attend_kernel(layer, steps, normalizer, *refs):
    core_ref, start_ref, startv_ref, cos_ref, sin_ref, ln_ref, qk_ref, ar_ref, *refs = refs
    if layer == 0:
        wq_hbm, wk_hbm, wv_hbm, k_hbm, v_hbm, *refs = refs
    else:
        prev_ref, wq_hbm, wk_hbm, wv_hbm, k_hbm, v_hbm, _, _, *refs = refs
    hid_ref, heads_ref, fresh_hbm, ko_hbm, vo_hbm, wq, wk, wv, qs, fresh, os, wsem, fsem, kbuf, vbuf, rsem, osem = refs
    heads = wq.shape[1] // HEAD
    half = qs.shape[1] // TILE
    nblk = half // NB
    hrows = half * steps
    core = core_ref[0]
    ln = lambda l, j: ln_ref[4 * l + j:4 * l + j + 1, :]
    weights = [(wq_hbm, wq), (wk_hbm, wk), (wv_hbm, wv)]
    wcopies = [pltpu.make_async_copy(src.at[layer], dst, wsem.at[n]) for n, (src, dst) in enumerate(weights)]
    stream = Stream(layer, core * half, (k_hbm, v_hbm), (ko_hbm, vo_hbm), (kbuf, vbuf), rsem, osem)
    for c in wcopies:
        c.start()
    stream.begin()

    if layer == 0:
        hid = ar_ref[...] * normalizer
    else:
        hid = prev_ref[...] + rms(ar_ref[...], ln(layer - 1, 3))
    hid_ref[...] = hid
    qs[...] = jnp.zeros_like(qs)
    fresh[...] = jnp.zeros_like(fresh)
    act = rms(hid, ln(layer, 0)).astype(BF16)
    for c in wcopies:
        c.wait()

    def roped(x, weight, at):
        x = rms(x, weight)
        a, b = x[:, :LANES], x[:, LANES:]
        c, s = cos_ref[at, :], sin_ref[at, :]
        return a * c - b * s, b * c + a * s

    def put_fresh(kv, pair):
        for c in range(2):
            for t in range(steps):
                r = c * hrows + t * half
                for g in range(2):
                    fresh[2 * kv + g, pl.ds(c * half * TILE + t, half, stride=TILE), :] = pair[g][r:r + half, :]

    k = jnp.dot(act, wk[...], preferred_element_type=F32)
    put_fresh(0, roped(k, qk_ref[2 * layer + 1:2 * layer + 2, :], slice(None)))
    v = jnp.dot(act, wv[...], preferred_element_type=F32)
    put_fresh(1, (v[:, :LANES], v[:, LANES:]))
    away = pl.ds(pl.multiple_of((1 - core) * half * TILE, TILE), half * TILE)
    keep = pltpu.make_async_copy(fresh.at[:, away, :], fresh_hbm, fsem)

    mine = pl.ds(pl.multiple_of(core * hrows, 8), hrows)
    own = rms(hid_ref[mine, :], ln(layer, 0)).astype(BF16)
    for h in range(heads):
        q = jnp.dot(own, wq[:, h * HEAD:(h + 1) * HEAD], preferred_element_type=F32)
        pair = roped(q, qk_ref[2 * layer:2 * layer + 1, :], mine)
        for g in range(2):
            for t in range(steps):
                qs[g, pl.ds(t * heads + h, half, stride=TILE), :] = pair[g][t * half:(t + 1) * half, :]

    scale = HEAD ** -0.5
    m_rows = NB * TILE

    def body(i, slot):
        at = tiles(i)
        gat = tiles(core * nblk + i)
        qb = wide(qs, 0, at).astype(BF16)
        kf = wide(fresh, 0, gat)
        vf = wide(fresh, 2, gat)
        start = startv_ref[gat, :]
        row = lax.broadcasted_iota(jnp.int32, (m_rows, LANES), 0)
        lane = lax.broadcasted_iota(jnp.int32, (m_rows, LANES), 1)
        t = lax.shift_right_logical(row & (TILE - 1), 2)
        old = jnp.concatenate([lax.dot_general(qb[TILE * j:TILE * (j + 1), :], kbuf[slot, j], NT, preferred_element_type=F32) for j in range(NB)], axis=0) * scale
        new = lax.dot_general(qb, kf.astype(BF16), NT, preferred_element_type=F32) * scale
        cols = []
        for g in range(0, WINDOW, LANES):
            s = lane + g
            ok = (s <= start + t) & (((s - start) & (WINDOW - 1)) > t)
            cols.append(jnp.where(ok, old[:, g:g + LANES], NEG))
        ok = (row - (row & (TILE - 1)) == lane - (lane & (TILE - 1))) & ((lane & (TILE - 1)) <= t)
        cols.append(jnp.where(ok, new, NEG))
        top = functools.reduce(jnp.maximum, cols)
        top = jnp.max(top, axis=-1, keepdims=True)
        exps = [jnp.exp(c - top) for c in cols]
        tot = jnp.sum(functools.reduce(jnp.add, exps), axis=-1, keepdims=True)
        inv = 1.0 / tot
        pold = jnp.concatenate([(e * inv).astype(BF16) for e in exps[:-1]], axis=1)
        pnew = (exps[-1] * inv).astype(BF16)
        out = jnp.dot(pnew, vf.astype(BF16), preferred_element_type=F32)
        out = out + jnp.concatenate([jnp.dot(pold[TILE * j:TILE * (j + 1), :], vbuf[slot, j], preferred_element_type=F32) for j in range(NB)], axis=0)
        os[0, at, :] = out[:, :LANES]
        os[1, at, :] = out[:, LANES:]
        stream.change(i, slot, start_ref, (kf, vf), steps)

    keep.start()
    stream.run(nblk, body)
    for h in range(heads):
        for g in range(2):
            for t in range(steps):
                value = os[g, pl.ds(t * heads + h, half, stride=TILE), :].astype(BF16).astype(F32)
                col = h * HEAD + g * LANES
                heads_ref[t * half:(t + 1) * half, col:col + LANES] = value
    keep.wait()
    stream.end(nblk)


def attend(layer, small, ar, prev, weights, caches, outs):
    batch = caches[0].shape[1]
    rows, dim = ar.shape
    half = batch // 2
    inner = weights[0].shape[2]
    normalizer = float(np.float32(dim ** 0.5).astype(BF16))
    ins = list(small) + [ar] + ([] if prev is None else [prev]) + list(weights) + list(caches)
    specs = [sspec()] * 2 + [vspec()] * (len(ins) - 7) + [aspec()] * 5
    alias = {}
    if outs is not None:
        alias = {len(ins): 3, len(ins) + 1: 4}
        ins += list(outs)
        specs += [aspec()] * 2
    return pl.pallas_call(
        functools.partial(attend_kernel, layer, rows // batch, normalizer),
        out_shape=[jax.ShapeDtypeStruct((rows, dim), F32), jax.ShapeDtypeStruct((rows // 2, inner), F32),
                   jax.ShapeDtypeStruct((4, half * TILE, LANES), F32)] + cache_shapes(caches),
        in_specs=specs,
        out_specs=[vspec(), vspec()] + [aspec()] * 3,
        scratch_shapes=[
            pltpu.VMEM((dim, inner), BF16), pltpu.VMEM((dim, HEAD), BF16), pltpu.VMEM((dim, HEAD), BF16),
            pltpu.VMEM((2, half * TILE, LANES), F32), pltpu.VMEM((4, batch * TILE, LANES), F32), pltpu.VMEM((2, half * TILE, LANES), F32),
            pltpu.SemaphoreType.DMA((3,)), pltpu.SemaphoreType.DMA,
        ] + stream_scratch(),
        input_output_aliases=alias,
        compiler_params=pltpu.CompilerParams(vmem_limit_bytes=42 * MIB),
        name=f"attend{layer}",
    )(*ins)


TV = 1024
EBUF = 8


def scores_kernel(nblk, ar_ref, prev_ref, ln_ref, nf_ref, tgt_ref, e_hbm, out_ref, f_ref, ebuf, za, zb, m_ref, s_ref, t_ref, sem):
    rows, dim = f_ref.shape

    def fetch(i, slot):
        return pltpu.make_async_copy(e_hbm.at[pl.ds(pl.multiple_of(i * TV, TV), TV), :], ebuf.at[slot], sem.at[slot])

    for i in range(EBUF - 2):
        fetch(i, i).start()
    hid = prev_ref[...] + rms(ar_ref[...], ln_ref[7:8, :])
    f_ref[...] = rms(hid, nf_ref[...]).astype(BF16)
    m_ref[...] = jnp.full_like(m_ref, -jnp.inf)
    s_ref[...] = jnp.zeros_like(s_ref)
    t_ref[...] = jnp.zeros_like(t_ref)

    def dots(slot, z):
        for c in range(TV // 256):
            z[:, c * 256:(c + 1) * 256] = lax.dot_general(f_ref[...], ebuf[slot, c * 256:(c + 1) * 256, :], NT, preferred_element_type=F32)

    def fold(i, z):
        for r in range(rows // 8):
            sl = slice(r * 8, (r + 1) * 8)
            vals = [z[sl, g * 128:(g + 1) * 128] for g in range(TV // 128)]
            top = m_ref[sl, :]
            tops = list(vals)
            while len(tops) > 1:
                tops = [jnp.maximum(tops[n], tops[n + 1]) for n in range(0, len(tops), 2)]
            new = jnp.maximum(top, tops[0])
            m_ref[sl, :] = new
            exps = [jnp.exp(v - new) for v in vals]
            while len(exps) > 1:
                exps = [exps[n] + exps[n + 1] for n in range(0, len(exps), 2)]
            s_ref[sl, :] = s_ref[sl, :] * jnp.exp(top - new) + exps[0]
            want = tgt_ref[sl, :]
            hit = t_ref[sl, :]
            for g, v in enumerate(vals):
                hit = jnp.where(want == i * TV + g * 128, v, hit)
            t_ref[sl, :] = hit

    def prep(i, slot):
        fetch(i, slot).wait()

    def more(i):
        @pl.when(i < nblk)
        def _():
            fetch(i, lax.rem(i, EBUF)).start()

    fetch(0, 0).wait()
    more(EBUF - 2)
    dots(0, za)

    def pair(n, carry):
        a = 2 * n + 1
        b = a + 1
        prep(a, lax.rem(a, EBUF))
        prep(b, lax.rem(b, EBUF))
        more(a + EBUF - 2)
        more(b + EBUF - 2)
        dots(lax.rem(a, EBUF), zb)
        fold(a - 1, za)
        dots(lax.rem(b, EBUF), za)
        fold(a, zb)
        return carry

    lax.fori_loop(0, (nblk - 2) // 2, pair, 0)
    last = nblk - 1
    prep(last, last % EBUF)
    dots(last % EBUF, zb)
    fold(last - 1, za)
    fold(last, zb)

    m = m_ref[...]
    top = jnp.max(m, axis=-1, keepdims=True)
    tot = jnp.sum(s_ref[...] * jnp.exp(m - top), axis=-1, keepdims=True)
    tgt = jnp.sum(t_ref[...], axis=-1, keepdims=True)
    lane = lax.broadcasted_iota(jnp.int32, (rows, 128), 1)
    pack = jnp.where(lane == 0, top, jnp.where(lane == 1, tot, jnp.where(lane == 2, tgt, 0.0)))
    pad = out_ref.shape[1] - rows
    pack = jnp.concatenate([pack, jnp.zeros((pad, 128), F32)], axis=0)
    out_ref[...] = jnp.transpose(pack)[:8, :]


def table_scores(ar, prev, ln, nf, tgt, table):
    rows, dim = ar.shape
    nblk = table.shape[0] // TV
    lanes = -(-rows // 128) * 128
    return pl.pallas_call(
        functools.partial(scores_kernel, nblk),
        out_shape=jax.ShapeDtypeStruct((8, lanes), F32),
        in_specs=[vspec()] * 5 + [aspec()],
        out_specs=vspec(),
        scratch_shapes=[
            pltpu.VMEM((rows, dim), BF16), pltpu.VMEM((EBUF, TV, dim), BF16),
            pltpu.VMEM((rows, TV), F32), pltpu.VMEM((rows, TV), F32),
            pltpu.VMEM((rows, 128), F32), pltpu.VMEM((rows, 128), F32), pltpu.VMEM((rows, 128), F32),
            pltpu.SemaphoreType.DMA((EBUF,)),
        ],
        compiler_params=pltpu.CompilerParams(vmem_limit_bytes=32 * MIB),
        name="table_scores",
    )(ar, prev, ln, nf, tgt, table)


def combine_kernel(x_ref, out_ref, got, ssem, rsem):
    dp = lax.axis_index("dp")
    tp = lax.axis_index("tp")
    barrier = pltpu.get_barrier_semaphore()
    for d in range(1, 4):
        pl.semaphore_signal(barrier, inc=1, device_id=(dp, lax.rem(tp + d, 4)), device_id_type=MESH)
    pl.semaphore_wait(barrier, 3)
    sends = []
    for d in range(1, 4):
        sends.append(pltpu.make_async_remote_copy(src_ref=x_ref, dst_ref=got.at[d - 1], send_sem=ssem.at[d - 1], recv_sem=rsem.at[d - 1],
                                                  device_id=(dp, lax.rem(tp + d, 4)), device_id_type=MESH))
        sends[-1].start()
    for s in sends:
        s.wait()
    mine = x_ref[...]
    vals = [mine] + [got[d] for d in range(3)]
    ordered = []
    for dev in range(4):
        v = mine
        for d in range(1, 4):
            v = jnp.where(lax.rem(tp + 4 - d, 4) == dev, vals[d], v)
        ordered.append(v)
    top = jnp.maximum(jnp.maximum(ordered[0][0:1], ordered[1][0:1]), jnp.maximum(ordered[2][0:1], ordered[3][0:1]))
    tot = 0.0
    tgt = 0.0
    for v in ordered:
        tot = tot + v[1:2] * jnp.exp(v[0:1] - top)
        tgt = tgt + v[2:3]
    log_z = top + jnp.log(tot)
    lanes = out_ref.shape[1]
    row = lax.broadcasted_iota(jnp.int32, (8, lanes), 0)
    out_ref[...] = jnp.where(row == 0, tgt - log_z, log_z)


def combine(x, cid):
    return pl.pallas_call(
        combine_kernel,
        out_shape=jax.ShapeDtypeStruct(x.shape, F32),
        in_specs=[vspec()],
        out_specs=vspec(),
        scratch_shapes=[pltpu.VMEM((3,) + x.shape, F32), pltpu.SemaphoreType.DMA((3,)), pltpu.SemaphoreType.DMA((3,))],
        compiler_params=pltpu.CompilerParams(collective_id=cid, has_side_effects=True),
        name="combine_tp",
    )(x)


def solution(mesh):
    arg_specs = (P('dp', None), P('dp', None), P('dp'), P('tp', None), P(), P(), P(), P(), P(), P(), P(None, None, 'tp'), P(None, None, 'tp'), P(None, 'tp', None), P(), P(None, 'dp'), P(None, 'dp'))
    result_specs = (P('dp', None), P('dp', None), P(None, 'dp'), P(None, 'dp'))

    def decode_local(tokens, targets, start_pos, embed_table, layer_norms, w_q, w_k, w_v, qk_norms, w_o, w_gate, w_up, w_down, norm_final, k_cache, v_cache):
        batch, steps = tokens.shape
        layers, dim, heads, head_dim = w_q.shape
        window = k_cache.shape[2]
        vocab_local = embed_table.shape[0]
        rows = batch * steps
        vocab_start = lax.axis_index('tp') * vocab_local
        def by_row(x):
            return jnp.swapaxes(x.reshape(2, batch // 2, steps), 1, 2).reshape(rows)

        def from_row(x):
            return jnp.swapaxes(x.reshape(2, steps, batch // 2), 1, 2).reshape(batch, steps)

        core = (lax.axis_index('tp') % 2).reshape(1)
        positions = by_row(start_pos[:, None] + jnp.arange(steps)[None, :])
        inv_freq = ROPE_BASE ** (-2.0 * jnp.arange(head_dim // 2, dtype=F32) / head_dim)
        angles = positions.astype(F32)[:, None] * inv_freq[None, :]
        startv = jnp.broadcast_to(start_pos[:, None, None], (batch, 16, 128)).reshape(batch * 16, 128)
        ln = layer_norms.reshape(layers * 4, dim)
        small = (core, start_pos, startv, jnp.cos(angles), jnp.sin(angles), ln, qk_norms.reshape(layers * 2, head_dim))
        qkv = (w_q.reshape(layers, dim, heads * head_dim), w_k.reshape(layers, dim, head_dim), w_v.reshape(layers, dim, head_dim))
        ffn = (w_o.reshape(layers, heads * head_dim, dim), jnp.swapaxes(w_gate, 1, 2), jnp.swapaxes(w_up, 1, 2), w_down)
        caches = (k_cache.reshape(layers, batch, window, head_dim), v_cache.reshape(layers, batch, window, head_dim))
        ar = share(pair_sum(gather_rows(by_row(tokens) - vocab_start, embed_table), 0), 1)
        hid, outs = None, None
        for layer in range(layers):
            hid, own_heads, fresh, *outs = attend(layer, small, ar, hid, qkv, caches, outs)
            hid, half = feed(layer, own_heads, hid, ln, ffn, 2 + layer)
            outs = carry_other(layer, steps, core, start_pos, fresh, caches, outs)
            ar = share(half, 4 + layer)
        tgt = (by_row(targets) - vocab_start)[:, None] - jnp.arange(LANES)[None, :]
        stats = table_scores(ar, hid, ln, norm_final.reshape(1, dim), tgt, embed_table)
        res = combine(stats, 4 + layers)
        return from_row(res[0, :rows]), from_row(res[1, :rows]), outs[0].reshape(k_cache.shape), outs[1].reshape(v_cache.shape)

    return jax.shard_map(decode_local, mesh=mesh, in_specs=arg_specs, out_specs=result_specs, check_vma=False)
```

```python
import functools

import jax
import jax.numpy as jnp
import numpy as np
from jax import lax
from jax.experimental import pallas as pl
from jax.experimental.pallas import tpu as pltpu
from jax.sharding import PartitionSpec as P

EPSILON = 1e-6
ROPE_BASE = 10000.0
NEG = -1e30
MESH = pl.DeviceIdType.MESH
F32 = jnp.float32
BF16 = jnp.bfloat16
NT = (((1,), (1,)), ((), ()))


def rms(values, weight):
    mean_sq = jnp.mean(values * values, axis=-1, keepdims=True)
    return values * lax.rsqrt(mean_sq + EPSILON) * (1.0 + weight)


def vspec():
    return pl.BlockSpec(memory_space=pltpu.VMEM)


def aspec():
    return pl.BlockSpec(memory_space=pl.ANY)


def sspec():
    return pl.BlockSpec(memory_space=pltpu.SMEM)


def gather_kernel(rows, grp_ref, col_ref, table_ref, out_ref, xbuf, sem):
    def issue(i, carry):
        src = pl.multiple_of(grp_ref[i] * 8, 8)
        dst = pl.multiple_of(i * 8, 8)
        pltpu.make_async_copy(table_ref.at[pl.ds(src, 8), :], xbuf.at[pl.ds(dst, 8), :], sem).start()
        return carry

    lax.fori_loop(0, rows, issue, 0, unroll=8)
    pltpu.make_async_copy(table_ref.at[pl.ds(0, rows * 8), :], xbuf, sem).wait()
    for c in range(rows // 32):
        lanes = lax.broadcasted_iota(jnp.int32, (32, 256), 1)
        pick = jnp.where(lanes == col_ref[c * 32:(c + 1) * 32, :], 1.0, 0.0).astype(BF16)
        out_ref[c * 32:(c + 1) * 32, :] = jnp.dot(pick, xbuf[c * 256:(c + 1) * 256, :], preferred_element_type=F32)


def gather_rows(ids, table):
    rows = ids.shape[0]
    vocab_local, dim = table.shape
    here = (ids >= 0) & (ids < vocab_local)
    safe = ids % vocab_local
    col = jnp.where(here, (jnp.arange(rows) % 32) * 8 + safe % 8, -1)[:, None]
    return pl.pallas_call(
        functools.partial(gather_kernel, rows),
        out_shape=jax.ShapeDtypeStruct((rows, dim), F32),
        in_specs=[sspec(), vspec(), aspec()],
        out_specs=vspec(),
        scratch_shapes=[pltpu.VMEM((rows * 8, dim), BF16), pltpu.SemaphoreType.DMA],
        compiler_params=pltpu.CompilerParams(vmem_limit_bytes=24 * 1024 * 1024),
        name="token_rows",
    )(safe // 8, col, table)


LANES = 128
HEAD = 2 * LANES
TILE = 16
WINDOW = 512
MIB = 1024 * 1024


def mate_of():
    tp = lax.axis_index("tp")
    core = lax.rem(tp, 2)
    return core, (lax.axis_index("dp"), tp + 1 - 2 * core)


def meet(mate):
    barrier = pltpu.get_barrier_semaphore()
    pl.semaphore_signal(barrier, inc=1, device_id=mate, device_id_type=MESH)
    pl.semaphore_wait(barrier, 1)


def send(src, dst, ssem, rsem, peer):
    return pltpu.make_async_remote_copy(src_ref=src, dst_ref=dst, send_sem=ssem, recv_sem=rsem, device_id=peer, device_id_type=MESH)


def part_rows(which, ref):
    hrows = ref.shape[0] // 2
    return pl.ds(pl.multiple_of(which * hrows, 8), hrows)


def mate_sum(part_ref, out_ref, got, ssem, rsem, core, mate):
    swap = send(part_ref.at[part_rows(1 - core, part_ref), :], got, ssem, rsem, mate)
    swap.start()
    swap.wait()
    out_ref[...] = part_ref[part_rows(core, part_ref), :] + got[...]


def pair_sum_kernel(part_ref, out_ref, got, ssem, rsem):
    core, mate = mate_of()
    meet(mate)
    mate_sum(part_ref, out_ref, got, ssem, rsem, core, mate)


def pair_share_kernel(a_ref, b_ref, out_ref, total, got, ssem, rsem):
    core, mate = mate_of()
    total[...] = a_ref[...] + b_ref[...]
    meet(mate)
    swap = send(total, got, ssem, rsem, mate)
    swap.start()
    out_ref[part_rows(core, out_ref), :] = total[...]
    swap.wait()
    out_ref[part_rows(1 - core, out_ref), :] = got[...]


def pair_call(kernel, out_rows, ins, scratch, cid, name):
    dim = ins[0].shape[1]
    return pl.pallas_call(
        kernel,
        out_shape=jax.ShapeDtypeStruct((out_rows, dim), F32),
        in_specs=[vspec()] * len(ins),
        out_specs=vspec(),
        scratch_shapes=[pltpu.VMEM(shape, F32) for shape in scratch] + [pltpu.SemaphoreType.DMA] * 2,
        compiler_params=pltpu.CompilerParams(collective_id=cid, has_side_effects=True, vmem_limit_bytes=12 * MIB),
        name=name,
    )(*ins)


def pair_sum(part, cid):
    rows, dim = part.shape
    return pair_call(pair_sum_kernel, rows // 2, [part], [(rows // 2, dim)], cid, "pair_sum")


def share(half, cid):
    far = lax.ppermute(half, 'tp', [(n, (n + 2) % 4) for n in range(4)])
    return pair_call(pair_share_kernel, half.shape[0] * 2, [half, far], [half.shape] * 2, cid, "pair_share")


NB = 8
NBUF = 6


class Stream:
    def __init__(self, layer, base, sources, targets, bufs, rsem, osem):
        self.layer, self.base = layer, base
        self.sources, self.targets, self.bufs, self.rsem, self.osem = sources, targets, bufs, rsem, osem

    def rows(self, i):
        return pl.ds(pl.multiple_of(self.base + i * NB, NB), NB)

    def reads(self, i, slot):
        return [pltpu.make_async_copy(src.at[self.layer, self.rows(i)], buf.at[slot], self.rsem.at[n, slot])
                for n, (src, buf) in enumerate(zip(self.sources, self.bufs))]

    def writes(self, i, slot):
        return [pltpu.make_async_copy(buf.at[slot], dst.at[self.layer, self.rows(i)], self.osem.at[n, slot])
                for n, (dst, buf) in enumerate(zip(self.targets, self.bufs))]

    def begin(self):
        for i in range(NBUF):
            for c in self.reads(i, i):
                c.start()

    def run(self, nblk, body):
        assert nblk == NBUF

        def block(i, carry):
            slot = i
            for c in self.reads(i, slot):
                c.wait()

            @pl.when(i >= 1)
            def _():
                for c in self.writes(i - 1, i - 1):
                    c.start()

            body(i, slot)
            return carry

        lax.fori_loop(0, nblk, block, 0)
        for c in self.writes(nblk - 1, nblk - 1):
            c.start()

    def end(self, nblk):
        for i in range(nblk):
            for c in self.writes(i, i):
                c.wait()

    def change(self, i, slot, start_ref, fresh, steps):
        sub = lax.broadcasted_iota(jnp.int32, (TILE, HEAD), 0)
        for first in (0, NB // 2):
            pending = []
            for j in range(first, first + NB // 2):
                st = start_ref[self.base + i * NB + j]
                for s in (st & (WINDOW - 1), (st + steps - 1) & (WINDOW - 1)):
                    at = pl.multiple_of(s - (s & (TILE - 1)), TILE)
                    dist = (sub + at - st) & (WINDOW - 1)
                    for buf, new in zip(self.bufs, fresh):
                        value = buf[slot, j, pl.ds(at, TILE), :].astype(F32)
                        for t in range(steps):
                            value = jnp.where(dist == t, new[TILE * j + t:TILE * j + t + 1, :], value)
                        pending.append((buf, j, at, value.astype(BF16)))
            for buf, j, at, value in pending:
                buf[slot, j, pl.ds(at, TILE), :] = value


def stream_scratch():
    buf = pltpu.VMEM((NBUF, NB, WINDOW, HEAD), BF16)
    sem = pltpu.SemaphoreType.DMA((2, NBUF))
    return [buf, buf, sem, sem]


def cache_shapes(caches):
    return [jax.ShapeDtypeStruct(c.shape, c.dtype) for c in caches]


def wide(ref, n, at):
    return jnp.concatenate([ref[n, at, :], ref[n + 1, at, :]], axis=1)


def tiles(i):
    return pl.ds(pl.multiple_of(i * NB * TILE, NB * TILE), NB * TILE)


def carry_kernel(layer, steps, core_ref, start_ref, fresh, k_hbm, v_hbm, _k, _v, ko_hbm, vo_hbm, kbuf, vbuf, rsem, osem):
    half = fresh.shape[1] // TILE
    nblk = half // NB
    stream = Stream(layer, (1 - core_ref[0]) * half, (k_hbm, v_hbm), (ko_hbm, vo_hbm), (kbuf, vbuf), rsem, osem)
    stream.begin()
    stream.run(nblk, lambda i, slot: stream.change(i, slot, start_ref, (wide(fresh, 0, tiles(i)), wide(fresh, 2, tiles(i))), steps))
    stream.end(nblk)


def carry_other(layer, steps, core, start, fresh, caches, outs):
    return pl.pallas_call(
        functools.partial(carry_kernel, layer, steps),
        out_shape=cache_shapes(caches),
        in_specs=[sspec(), sspec(), vspec()] + [aspec()] * 4,
        out_specs=[aspec()] * 2,
        scratch_shapes=stream_scratch(),
        input_output_aliases={5: 0, 6: 1},
        compiler_params=pltpu.CompilerParams(vmem_limit_bytes=32 * MIB),
        cost_estimate=pl.CostEstimate(flops=10 ** 10, bytes_accessed=48 * MIB, transcendentals=0),
        name=f"carry{layer}",
    )(core, start, fresh, *caches, *outs)


def feed_kernel(layer, heads_ref, hid_ref, ln_ref, wo_hbm, wg_hbm, wu_hbm, wd_hbm,
                hid_out, half_ref, wo, wg, wu, wd, both, part, got, wsem, hsend, hrecv, ssem, rsem):
    core, mate = mate_of()
    weights = [(wo_hbm, wo), (wg_hbm, wg), (wu_hbm, wu), (wd_hbm, wd)]
    wcopies = [pltpu.make_async_copy(src.at[layer], dst, wsem.at[n]) for n, (src, dst) in enumerate(weights)]
    for c in wcopies:
        c.start()
    meet(mate)
    swap = send(heads_ref, both.at[core], hsend, hrecv, mate)
    swap.start()
    both[core] = heads_ref[...]
    ln = lambda j: ln_ref[4 * layer + j:4 * layer + j + 1, :]
    wcopies[0].wait()
    swap.wait_recv()
    x = jnp.concatenate([both[0], both[1]], axis=0).astype(BF16)
    hid = hid_ref[...] + rms(jnp.dot(x, wo[...], preferred_element_type=F32), ln(1))
    hid_out[...] = hid
    act = rms(hid, ln(2)).astype(BF16)
    for c in wcopies[1:]:
        c.wait()
    width = wg.shape[0]
    for at in range(0, width, WINDOW):
        cut = slice(at, min(at + WINDOW, width))
        gate = lax.dot_general(act, wg[cut, :], NT, preferred_element_type=F32)
        up = lax.dot_general(act, wu[cut, :], NT, preferred_element_type=F32)
        inner = (jax.nn.gelu(gate, approximate=True) * up).astype(BF16)
        down = jnp.dot(inner, wd[cut, :], preferred_element_type=F32)
        if at == 0:
            part[...] = down
        else:
            part[...] += down
    swap.wait_send()
    mate_sum(part, half_ref, got, ssem, rsem, core, mate)


def feed(layer, heads, hid, ln, weights, cid):
    rows, dim = hid.shape
    width = weights[1].shape[1]
    own, inner = heads.shape
    return pl.pallas_call(
        functools.partial(feed_kernel, layer),
        out_shape=[jax.ShapeDtypeStruct((rows, dim), F32), jax.ShapeDtypeStruct((own, dim), F32)],
        in_specs=[vspec()] * 3 + [aspec()] * 4,
        out_specs=[vspec()] * 2,
        scratch_shapes=[pltpu.VMEM((inner, dim), BF16)] + [pltpu.VMEM((width, dim), BF16)] * 3 + [
            pltpu.VMEM((2, own, inner), F32), pltpu.VMEM((rows, dim), F32), pltpu.VMEM((own, dim), F32),
            pltpu.SemaphoreType.DMA((4,))] + [pltpu.SemaphoreType.DMA] * 4,
        compiler_params=pltpu.CompilerParams(collective_id=cid, has_side_effects=True, vmem_limit_bytes=40 * MIB),
        name=f"feed{layer}",
    )(heads, hid, ln, *weights)


def attend_kernel(layer, steps, normalizer, *refs):
    core_ref, start_ref, startv_ref, cos_ref, sin_ref, ln_ref, qk_ref, ar_ref, *refs = refs
    if layer == 0:
        wq_hbm, wk_hbm, wv_hbm, k_hbm, v_hbm, *refs = refs
    else:
        prev_ref, wq_hbm, wk_hbm, wv_hbm, k_hbm, v_hbm, _, _, *refs = refs
    hid_ref, heads_ref, fresh_hbm, ko_hbm, vo_hbm, wq, wk, wv, qs, fresh, os, wsem, fsem, kbuf, vbuf, rsem, osem = refs
    heads = wq.shape[1] // HEAD
    half = qs.shape[1] // TILE
    nblk = half // NB
    hrows = half * steps
    core = core_ref[0]
    ln = lambda l, j: ln_ref[4 * l + j:4 * l + j + 1, :]
    weights = [(wq_hbm, wq), (wk_hbm, wk), (wv_hbm, wv)]
    wcopies = [pltpu.make_async_copy(src.at[layer], dst, wsem.at[n]) for n, (src, dst) in enumerate(weights)]
    stream = Stream(layer, core * half, (k_hbm, v_hbm), (ko_hbm, vo_hbm), (kbuf, vbuf), rsem, osem)
    for c in wcopies:
        c.start()
    stream.begin()

    if layer == 0:
        hid = ar_ref[...] * normalizer
    else:
        hid = prev_ref[...] + rms(ar_ref[...], ln(layer - 1, 3))
    hid_ref[...] = hid
    qs[...] = jnp.zeros_like(qs)
    fresh[...] = jnp.zeros_like(fresh)
    act = rms(hid, ln(layer, 0)).astype(BF16)
    for c in wcopies:
        c.wait()

    def roped(x, weight, at):
        x = rms(x, weight)
        a, b = x[:, :LANES], x[:, LANES:]
        c, s = cos_ref[at, :], sin_ref[at, :]
        return a * c - b * s, b * c + a * s

    def put_fresh(kv, pair):
        for c in range(2):
            for t in range(steps):
                r = c * hrows + t * half
                for g in range(2):
                    fresh[2 * kv + g, pl.ds(c * half * TILE + t, half, stride=TILE), :] = pair[g][r:r + half, :]

    k = jnp.dot(act, wk[...], preferred_element_type=F32)
    put_fresh(0, roped(k, qk_ref[2 * layer + 1:2 * layer + 2, :], slice(None)))
    v = jnp.dot(act, wv[...], preferred_element_type=F32)
    put_fresh(1, (v[:, :LANES], v[:, LANES:]))
    away = pl.ds(pl.multiple_of((1 - core) * half * TILE, TILE), half * TILE)
    keep = pltpu.make_async_copy(fresh.at[:, away, :], fresh_hbm, fsem)

    mine = pl.ds(pl.multiple_of(core * hrows, 8), hrows)
    own = rms(hid_ref[mine, :], ln(layer, 0)).astype(BF16)
    for h in range(heads):
        q = jnp.dot(own, wq[:, h * HEAD:(h + 1) * HEAD], preferred_element_type=F32)
        pair = roped(q, qk_ref[2 * layer:2 * layer + 1, :], mine)
        for g in range(2):
            for t in range(steps):
                qs[g, pl.ds(t * heads + h, half, stride=TILE), :] = pair[g][t * half:(t + 1) * half, :]

    scale = HEAD ** -0.5
    m_rows = NB * TILE

    def body(i, slot):
        at = tiles(i)
        gat = tiles(core * nblk + i)
        qb = wide(qs, 0, at).astype(BF16)
        kf = wide(fresh, 0, gat)
        vf = wide(fresh, 2, gat)
        start = startv_ref[gat, :]
        row = lax.broadcasted_iota(jnp.int32, (m_rows, LANES), 0)
        lane = lax.broadcasted_iota(jnp.int32, (m_rows, LANES), 1)
        t = lax.shift_right_logical(row & (TILE - 1), 2)
        old = jnp.concatenate([lax.dot_general(qb[TILE * j:TILE * (j + 1), :], kbuf[slot, j], NT, preferred_element_type=F32) for j in range(NB)], axis=0) * scale
        new = lax.dot_general(qb, kf.astype(BF16), NT, preferred_element_type=F32) * scale
        cols = []
        for g in range(0, WINDOW, LANES):
            s = lane + g
            ok = (s <= start + t) & (((s - start) & (WINDOW - 1)) > t)
            cols.append(jnp.where(ok, old[:, g:g + LANES], NEG))
        ok = (row - (row & (TILE - 1)) == lane - (lane & (TILE - 1))) & ((lane & (TILE - 1)) <= t)
        cols.append(jnp.where(ok, new, NEG))
        top = functools.reduce(jnp.maximum, cols)
        top = jnp.max(top, axis=-1, keepdims=True)
        exps = [jnp.exp(c - top) for c in cols]
        tot = jnp.sum(functools.reduce(jnp.add, exps), axis=-1, keepdims=True)
        inv = 1.0 / tot
        pold = jnp.concatenate([(e * inv).astype(BF16) for e in exps[:-1]], axis=1)
        pnew = (exps[-1] * inv).astype(BF16)
        out = jnp.dot(pnew, vf.astype(BF16), preferred_element_type=F32)
        out = out + jnp.concatenate([jnp.dot(pold[TILE * j:TILE * (j + 1), :], vbuf[slot, j], preferred_element_type=F32) for j in range(NB)], axis=0)
        os[0, at, :] = out[:, :LANES]
        os[1, at, :] = out[:, LANES:]
        stream.change(i, slot, start_ref, (kf, vf), steps)

    keep.start()
    stream.run(nblk, body)
    for h in range(heads):
        for g in range(2):
            for t in range(steps):
                value = os[g, pl.ds(t * heads + h, half, stride=TILE), :].astype(BF16).astype(F32)
                col = h * HEAD + g * LANES
                heads_ref[t * half:(t + 1) * half, col:col + LANES] = value
    keep.wait()
    stream.end(nblk)


def attend(layer, small, ar, prev, weights, caches, outs):
    batch = caches[0].shape[1]
    rows, dim = ar.shape
    half = batch // 2
    inner = weights[0].shape[2]
    normalizer = float(np.float32(dim ** 0.5).astype(BF16))
    ins = list(small) + [ar] + ([] if prev is None else [prev]) + list(weights) + list(caches)
    specs = [sspec()] * 2 + [vspec()] * (len(ins) - 7) + [aspec()] * 5
    alias = {}
    if outs is not None:
        alias = {len(ins): 3, len(ins) + 1: 4}
        ins += list(outs)
        specs += [aspec()] * 2
    return pl.pallas_call(
        functools.partial(attend_kernel, layer, rows // batch, normalizer),
        out_shape=[jax.ShapeDtypeStruct((rows, dim), F32), jax.ShapeDtypeStruct((rows // 2, inner), F32),
                   jax.ShapeDtypeStruct((4, half * TILE, LANES), F32)] + cache_shapes(caches),
        in_specs=specs,
        out_specs=[vspec(), vspec()] + [aspec()] * 3,
        scratch_shapes=[
            pltpu.VMEM((dim, inner), BF16), pltpu.VMEM((dim, HEAD), BF16), pltpu.VMEM((dim, HEAD), BF16),
            pltpu.VMEM((2, half * TILE, LANES), F32), pltpu.VMEM((4, batch * TILE, LANES), F32), pltpu.VMEM((2, half * TILE, LANES), F32),
            pltpu.SemaphoreType.DMA((3,)), pltpu.SemaphoreType.DMA,
        ] + stream_scratch(),
        input_output_aliases=alias,
        compiler_params=pltpu.CompilerParams(vmem_limit_bytes=50 * MIB),
        name=f"attend{layer}",
    )(*ins)


TV = 2048
EBUF = 6


def scores_kernel(nblk, ar_ref, prev_ref, ln_ref, nf_ref, tgt_ref, e_hbm, out_ref, f_ref, ebuf, za, zb, m_ref, s_ref, t_ref, sem):
    rows, dim = f_ref.shape

    def fetch(i, slot):
        return pltpu.make_async_copy(e_hbm.at[pl.ds(pl.multiple_of(i * TV, TV), TV), :], ebuf.at[slot], sem.at[slot])

    for i in range(EBUF - 2):
        fetch(i, i).start()
    hid = prev_ref[...] + rms(ar_ref[...], ln_ref[7:8, :])
    f_ref[...] = rms(hid, nf_ref[...]).astype(BF16)
    m_ref[...] = jnp.full_like(m_ref, -jnp.inf)
    s_ref[...] = jnp.zeros_like(s_ref)
    t_ref[...] = jnp.zeros_like(t_ref)

    def dots(slot, z):
        for c in range(TV // 256):
            z[:, c * 256:(c + 1) * 256] = lax.dot_general(f_ref[...], ebuf[slot, c * 256:(c + 1) * 256, :], NT, preferred_element_type=F32)

    def fold(i, z):
        for r in range(rows // 8):
            sl = slice(r * 8, (r + 1) * 8)
            vals = [z[sl, g * 128:(g + 1) * 128] for g in range(TV // 128)]
            top = m_ref[sl, :]
            tops = list(vals)
            while len(tops) > 1:
                tops = [jnp.maximum(tops[n], tops[n + 1]) for n in range(0, len(tops), 2)]
            new = jnp.maximum(top, tops[0])
            m_ref[sl, :] = new
            exps = [jnp.exp(v - new) for v in vals]
            while len(exps) > 1:
                exps = [exps[n] + exps[n + 1] for n in range(0, len(exps), 2)]
            s_ref[sl, :] = s_ref[sl, :] * jnp.exp(top - new) + exps[0]
            want = tgt_ref[sl, :]
            hit = t_ref[sl, :]
            for g, v in enumerate(vals):
                hit = jnp.where(want == i * TV + g * 128, v, hit)
            t_ref[sl, :] = hit

    def prep(i, slot):
        fetch(i, slot).wait()

    def more(i):
        @pl.when(i < nblk)
        def _():
            fetch(i, lax.rem(i, EBUF)).start()

    fetch(0, 0).wait()
    more(EBUF - 2)
    dots(0, za)

    def pair(n, carry):
        a = 2 * n + 1
        b = a + 1
        prep(a, lax.rem(a, EBUF))
        prep(b, lax.rem(b, EBUF))
        more(a + EBUF - 2)
        more(b + EBUF - 2)
        dots(lax.rem(a, EBUF), zb)
        fold(a - 1, za)
        dots(lax.rem(b, EBUF), za)
        fold(a, zb)
        return carry

    lax.fori_loop(0, (nblk - 2) // 2, pair, 0)
    last = nblk - 1
    prep(last, last % EBUF)
    dots(last % EBUF, zb)
    fold(last - 1, za)
    fold(last, zb)

    m = m_ref[...]
    top = jnp.max(m, axis=-1, keepdims=True)
    tot = jnp.sum(s_ref[...] * jnp.exp(m - top), axis=-1, keepdims=True)
    tgt = jnp.sum(t_ref[...], axis=-1, keepdims=True)
    lane = lax.broadcasted_iota(jnp.int32, (rows, 128), 1)
    pack = jnp.where(lane == 0, top, jnp.where(lane == 1, tot, jnp.where(lane == 2, tgt, 0.0)))
    pad = out_ref.shape[1] - rows
    pack = jnp.concatenate([pack, jnp.zeros((pad, 128), F32)], axis=0)
    out_ref[...] = jnp.transpose(pack)[:8, :]


def table_scores(ar, prev, ln, nf, tgt, table):
    rows, dim = ar.shape
    nblk = table.shape[0] // TV
    lanes = -(-rows // 128) * 128
    return pl.pallas_call(
        functools.partial(scores_kernel, nblk),
        out_shape=jax.ShapeDtypeStruct((8, lanes), F32),
        in_specs=[vspec()] * 5 + [aspec()],
        out_specs=vspec(),
        scratch_shapes=[
            pltpu.VMEM((rows, dim), BF16), pltpu.VMEM((EBUF, TV, dim), BF16),
            pltpu.VMEM((rows, TV), F32), pltpu.VMEM((rows, TV), F32),
            pltpu.VMEM((rows, 128), F32), pltpu.VMEM((rows, 128), F32), pltpu.VMEM((rows, 128), F32),
            pltpu.SemaphoreType.DMA((EBUF,)),
        ],
        compiler_params=pltpu.CompilerParams(vmem_limit_bytes=46 * MIB),
        name="table_scores",
    )(ar, prev, ln, nf, tgt, table)


def combine_kernel(x_ref, out_ref, got, ssem, rsem):
    dp = lax.axis_index("dp")
    tp = lax.axis_index("tp")
    barrier = pltpu.get_barrier_semaphore()
    for d in range(1, 4):
        pl.semaphore_signal(barrier, inc=1, device_id=(dp, lax.rem(tp + d, 4)), device_id_type=MESH)
    pl.semaphore_wait(barrier, 3)
    sends = []
    for d in range(1, 4):
        sends.append(pltpu.make_async_remote_copy(src_ref=x_ref, dst_ref=got.at[d - 1], send_sem=ssem.at[d - 1], recv_sem=rsem.at[d - 1],
                                                  device_id=(dp, lax.rem(tp + d, 4)), device_id_type=MESH))
        sends[-1].start()
    for s in sends:
        s.wait()
    mine = x_ref[...]
    vals = [mine] + [got[d] for d in range(3)]
    ordered = []
    for dev in range(4):
        v = mine
        for d in range(1, 4):
            v = jnp.where(lax.rem(tp + 4 - d, 4) == dev, vals[d], v)
        ordered.append(v)
    top = jnp.maximum(jnp.maximum(ordered[0][0:1], ordered[1][0:1]), jnp.maximum(ordered[2][0:1], ordered[3][0:1]))
    tot = 0.0
    tgt = 0.0
    for v in ordered:
        tot = tot + v[1:2] * jnp.exp(v[0:1] - top)
        tgt = tgt + v[2:3]
    log_z = top + jnp.log(tot)
    lanes = out_ref.shape[1]
    row = lax.broadcasted_iota(jnp.int32, (8, lanes), 0)
    out_ref[...] = jnp.where(row == 0, tgt - log_z, log_z)


def combine(x, cid):
    return pl.pallas_call(
        combine_kernel,
        out_shape=jax.ShapeDtypeStruct(x.shape, F32),
        in_specs=[vspec()],
        out_specs=vspec(),
        scratch_shapes=[pltpu.VMEM((3,) + x.shape, F32), pltpu.SemaphoreType.DMA((3,)), pltpu.SemaphoreType.DMA((3,))],
        compiler_params=pltpu.CompilerParams(collective_id=cid, has_side_effects=True),
        name="combine_tp",
    )(x)


def solution(mesh):
    arg_specs = (P('dp', None), P('dp', None), P('dp'), P('tp', None), P(), P(), P(), P(), P(), P(), P(None, None, 'tp'), P(None, None, 'tp'), P(None, 'tp', None), P(), P(None, 'dp'), P(None, 'dp'))
    result_specs = (P('dp', None), P('dp', None), P(None, 'dp'), P(None, 'dp'))

    def decode_local(tokens, targets, start_pos, embed_table, layer_norms, w_q, w_k, w_v, qk_norms, w_o, w_gate, w_up, w_down, norm_final, k_cache, v_cache):
        batch, steps = tokens.shape
        layers, dim, heads, head_dim = w_q.shape
        window = k_cache.shape[2]
        vocab_local = embed_table.shape[0]
        rows = batch * steps
        vocab_start = lax.axis_index('tp') * vocab_local
        def by_row(x):
            return jnp.swapaxes(x.reshape(2, batch // 2, steps), 1, 2).reshape(rows)

        def from_row(x):
            return jnp.swapaxes(x.reshape(2, steps, batch // 2), 1, 2).reshape(batch, steps)

        core = (lax.axis_index('tp') % 2).reshape(1)
        positions = by_row(start_pos[:, None] + jnp.arange(steps)[None, :])
        inv_freq = ROPE_BASE ** (-2.0 * jnp.arange(head_dim // 2, dtype=F32) / head_dim)
        angles = positions.astype(F32)[:, None] * inv_freq[None, :]
        startv = jnp.broadcast_to(start_pos[:, None, None], (batch, 16, 128)).reshape(batch * 16, 128)
        ln = layer_norms.reshape(layers * 4, dim)
        small = (core, start_pos, startv, jnp.cos(angles), jnp.sin(angles), ln, qk_norms.reshape(layers * 2, head_dim))
        qkv = (w_q.reshape(layers, dim, heads * head_dim), w_k.reshape(layers, dim, head_dim), w_v.reshape(layers, dim, head_dim))
        ffn = (w_o.reshape(layers, heads * head_dim, dim), jnp.swapaxes(w_gate, 1, 2), jnp.swapaxes(w_up, 1, 2), w_down)
        caches = (k_cache.reshape(layers, batch, window, head_dim), v_cache.reshape(layers, batch, window, head_dim))
        ar = share(pair_sum(gather_rows(by_row(tokens) - vocab_start, embed_table), 0), 1)
        hid, outs = None, None
        for layer in range(layers):
            hid, own_heads, fresh, *outs = attend(layer, small, ar, hid, qkv, caches, outs)
            hid, half = feed(layer, own_heads, hid, ln, ffn, 2 + layer)
            outs = carry_other(layer, steps, core, start_pos, fresh, caches, outs)
            ar = share(half, 4 + layer)
        tgt = (by_row(targets) - vocab_start)[:, None] - jnp.arange(LANES)[None, :]
        stats = table_scores(ar, hid, ln, norm_final.reshape(1, dim), tgt, embed_table)
        res = combine(stats, 4 + layers)
        return from_row(res[0, :rows]), from_row(res[1, :rows]), outs[0].reshape(k_cache.shape), outs[1].reshape(v_cache.shape)

    return jax.shard_map(decode_local, mesh=mesh, in_specs=arg_specs, out_specs=result_specs, check_vma=False)
```

```python
import functools

import jax
import jax.numpy as jnp
import numpy as np
from jax import lax
from jax.experimental import pallas as pl
from jax.experimental.pallas import tpu as pltpu
from jax.sharding import PartitionSpec as P

EPSILON = 1e-6
ROPE_BASE = 10000.0
NEG = -1e30
MESH = pl.DeviceIdType.MESH
F32 = jnp.float32
BF16 = jnp.bfloat16
NT = (((1,), (1,)), ((), ()))


def rms(values, weight):
    mean_sq = jnp.mean(values * values, axis=-1, keepdims=True)
    return values * lax.rsqrt(mean_sq + EPSILON) * (1.0 + weight)


def vspec():
    return pl.BlockSpec(memory_space=pltpu.VMEM)


def aspec():
    return pl.BlockSpec(memory_space=pl.ANY)


def sspec():
    return pl.BlockSpec(memory_space=pltpu.SMEM)


def gather_kernel(rows, grp_ref, col_ref, table_ref, out_ref, xbuf, sem):
    def issue(i, carry):
        src = pl.multiple_of(grp_ref[i] * 8, 8)
        dst = pl.multiple_of(i * 8, 8)
        pltpu.make_async_copy(table_ref.at[pl.ds(src, 8), :], xbuf.at[pl.ds(dst, 8), :], sem).start()
        return carry

    lax.fori_loop(0, rows, issue, 0, unroll=8)
    pltpu.make_async_copy(table_ref.at[pl.ds(0, rows * 8), :], xbuf, sem).wait()
    for c in range(rows // 32):
        lanes = lax.broadcasted_iota(jnp.int32, (32, 256), 1)
        pick = jnp.where(lanes == col_ref[c * 32:(c + 1) * 32, :], 1.0, 0.0).astype(BF16)
        out_ref[c * 32:(c + 1) * 32, :] = jnp.dot(pick, xbuf[c * 256:(c + 1) * 256, :], preferred_element_type=F32)


def gather_rows(ids, table):
    rows = ids.shape[0]
    vocab_local, dim = table.shape
    here = (ids >= 0) & (ids < vocab_local)
    safe = ids % vocab_local
    col = jnp.where(here, (jnp.arange(rows) % 32) * 8 + safe % 8, -1)[:, None]
    return pl.pallas_call(
        functools.partial(gather_kernel, rows),
        out_shape=jax.ShapeDtypeStruct((rows, dim), F32),
        in_specs=[sspec(), vspec(), aspec()],
        out_specs=vspec(),
        scratch_shapes=[pltpu.VMEM((rows * 8, dim), BF16), pltpu.SemaphoreType.DMA],
        compiler_params=pltpu.CompilerParams(vmem_limit_bytes=24 * 1024 * 1024),
        name="token_rows",
    )(safe // 8, col, table)


LANES = 128
HEAD = 2 * LANES
TILE = 16
WINDOW = 512
MIB = 1024 * 1024


def mate_of():
    tp = lax.axis_index("tp")
    core = lax.rem(tp, 2)
    return core, (lax.axis_index("dp"), tp + 1 - 2 * core)


def meet(mate):
    barrier = pltpu.get_barrier_semaphore()
    pl.semaphore_signal(barrier, inc=1, device_id=mate, device_id_type=MESH)
    pl.semaphore_wait(barrier, 1)


def send(src, dst, ssem, rsem, peer):
    return pltpu.make_async_remote_copy(src_ref=src, dst_ref=dst, send_sem=ssem, recv_sem=rsem, device_id=peer, device_id_type=MESH)


def part_rows(which, ref):
    hrows = ref.shape[0] // 2
    return pl.ds(pl.multiple_of(which * hrows, 8), hrows)


def mate_sum(part_ref, out_ref, got, ssem, rsem, core, mate):
    swap = send(part_ref.at[part_rows(1 - core, part_ref), :], got, ssem, rsem, mate)
    swap.start()
    swap.wait()
    out_ref[...] = part_ref[part_rows(core, part_ref), :] + got[...]


def pair_sum_kernel(part_ref, out_ref, got, ssem, rsem):
    core, mate = mate_of()
    meet(mate)
    mate_sum(part_ref, out_ref, got, ssem, rsem, core, mate)


def pair_share_kernel(a_ref, b_ref, out_ref, total, got, ssem, rsem):
    core, mate = mate_of()
    total[...] = a_ref[...] + b_ref[...]
    meet(mate)
    swap = send(total, got, ssem, rsem, mate)
    swap.start()
    out_ref[part_rows(core, out_ref), :] = total[...]
    swap.wait()
    out_ref[part_rows(1 - core, out_ref), :] = got[...]


def pair_call(kernel, out_rows, ins, scratch, cid, name):
    dim = ins[0].shape[1]
    return pl.pallas_call(
        kernel,
        out_shape=jax.ShapeDtypeStruct((out_rows, dim), F32),
        in_specs=[vspec()] * len(ins),
        out_specs=vspec(),
        scratch_shapes=[pltpu.VMEM(shape, F32) for shape in scratch] + [pltpu.SemaphoreType.DMA] * 2,
        compiler_params=pltpu.CompilerParams(collective_id=cid, has_side_effects=True, vmem_limit_bytes=12 * MIB),
        name=name,
    )(*ins)


def pair_sum(part, cid):
    rows, dim = part.shape
    return pair_call(pair_sum_kernel, rows // 2, [part], [(rows // 2, dim)], cid, "pair_sum")


def share(half, cid):
    far = lax.ppermute(half, 'tp', [(n, (n + 2) % 4) for n in range(4)])
    return pair_call(pair_share_kernel, half.shape[0] * 2, [half, far], [half.shape] * 2, cid, "pair_share")


NB = 8
NBUF = 4


class Stream:
    def __init__(self, layer, base, sources, targets, bufs, rsem, osem):
        self.layer, self.base = layer, base
        self.sources, self.targets, self.bufs, self.rsem, self.osem = sources, targets, bufs, rsem, osem

    def rows(self, i):
        return pl.ds(pl.multiple_of(self.base + i * NB, NB), NB)

    def reads(self, i, slot):
        return [pltpu.make_async_copy(src.at[self.layer, self.rows(i)], buf.at[slot], self.rsem.at[n, slot])
                for n, (src, buf) in enumerate(zip(self.sources, self.bufs))]

    def writes(self, i, slot):
        return [pltpu.make_async_copy(buf.at[slot], dst.at[self.layer, self.rows(i)], self.osem.at[n, slot])
                for n, (dst, buf) in enumerate(zip(self.targets, self.bufs))]

    def begin(self, first, last):
        for i in range(first, last):
            for c in self.reads(i, i):
                c.start()

    def run(self, nblk, body):
        def block(i, carry):
            slot = lax.rem(i, NBUF)
            for c in self.reads(i, slot):
                c.wait()

            @pl.when(i >= 1)
            def _():
                for c in self.writes(i - 1, lax.rem(i + NBUF - 1, NBUF)):
                    c.start()

            @pl.when(i >= 2)
            def _():
                for c in self.writes(i - 2, lax.rem(i + NBUF - 2, NBUF)):
                    c.wait()

            @pl.when((i + 2 >= NBUF) & (i + 2 < nblk))
            def _():
                for c in self.reads(i + 2, lax.rem(i + 2, NBUF)):
                    c.start()

            body(i, slot)
            return carry

        lax.fori_loop(0, nblk, block, 0)
        for c in self.writes(nblk - 1, (nblk - 1) % NBUF):
            c.start()

    def end(self, nblk):
        for i in (nblk - 2, nblk - 1):
            for c in self.writes(i, i % NBUF):
                c.wait()

    def change(self, i, slot, start_ref, fresh, steps):
        sub = lax.broadcasted_iota(jnp.int32, (TILE, HEAD), 0)
        for first in (0, NB // 2):
            pending = []
            for j in range(first, first + NB // 2):
                st = start_ref[self.base + i * NB + j]
                for s in (st & (WINDOW - 1), (st + steps - 1) & (WINDOW - 1)):
                    at = pl.multiple_of(s - (s & (TILE - 1)), TILE)
                    dist = (sub + at - st) & (WINDOW - 1)
                    for buf, new in zip(self.bufs, fresh):
                        value = buf[slot, j, pl.ds(at, TILE), :].astype(F32)
                        for t in range(steps):
                            value = jnp.where(dist == t, new[TILE * j + t:TILE * j + t + 1, :], value)
                        pending.append((buf, j, at, value.astype(BF16)))
            for buf, j, at, value in pending:
                buf[slot, j, pl.ds(at, TILE), :] = value


def stream_scratch():
    buf = pltpu.VMEM((NBUF, NB, WINDOW, HEAD), BF16)
    sem = pltpu.SemaphoreType.DMA((2, NBUF))
    return [buf, buf, sem, sem]


def cache_shapes(caches):
    return [jax.ShapeDtypeStruct(c.shape, c.dtype) for c in caches]


def wide(ref, n, at):
    return jnp.concatenate([ref[n, at, :], ref[n + 1, at, :]], axis=1)


def tiles(i):
    return pl.ds(pl.multiple_of(i * NB * TILE, NB * TILE), NB * TILE)


def carry_kernel(layer, steps, core_ref, start_ref, fresh, k_hbm, v_hbm, _k, _v, ko_hbm, vo_hbm, kbuf, vbuf, rsem, osem):
    half = fresh.shape[1] // TILE
    nblk = half // NB
    stream = Stream(layer, (1 - core_ref[0]) * half, (k_hbm, v_hbm), (ko_hbm, vo_hbm), (kbuf, vbuf), rsem, osem)
    stream.begin(0, NBUF)
    stream.run(nblk, lambda i, slot: stream.change(i, slot, start_ref, (wide(fresh, 0, tiles(i)), wide(fresh, 2, tiles(i))), steps))
    stream.end(nblk)


def carry_other(layer, steps, core, start, fresh, caches, outs):
    return pl.pallas_call(
        functools.partial(carry_kernel, layer, steps),
        out_shape=cache_shapes(caches),
        in_specs=[sspec(), sspec(), vspec()] + [aspec()] * 4,
        out_specs=[aspec()] * 2,
        scratch_shapes=stream_scratch(),
        input_output_aliases={5: 0, 6: 1},
        compiler_params=pltpu.CompilerParams(vmem_limit_bytes=24 * MIB),
        cost_estimate=pl.CostEstimate(flops=10 ** 10, bytes_accessed=48 * MIB, transcendentals=0),
        name=f"carry{layer}",
    )(core, start, fresh, *caches, *outs)


def feed_kernel(layer, heads_ref, hid_ref, ln_ref, wo_hbm, wg_hbm, wu_hbm, wd_hbm,
                hid_out, half_ref, wo, wg, wu, wd, both, part, got, wsem, hsend, hrecv, ssem, rsem):
    core, mate = mate_of()
    weights = [(wo_hbm, wo), (wg_hbm, wg), (wu_hbm, wu), (wd_hbm, wd)]
    wcopies = [pltpu.make_async_copy(src.at[layer], dst, wsem.at[n]) for n, (src, dst) in enumerate(weights)]
    for c in wcopies:
        c.start()
    meet(mate)
    swap = send(heads_ref, both.at[core], hsend, hrecv, mate)
    swap.start()
    both[core] = heads_ref[...]
    ln = lambda j: ln_ref[4 * layer + j:4 * layer + j + 1, :]
    wcopies[0].wait()
    swap.wait_recv()
    x = jnp.concatenate([both[0], both[1]], axis=0).astype(BF16)
    hid = hid_ref[...] + rms(jnp.dot(x, wo[...], preferred_element_type=F32), ln(1))
    hid_out[...] = hid
    act = rms(hid, ln(2)).astype(BF16)
    for c in wcopies[1:]:
        c.wait()
    width = wg.shape[0]
    for at in range(0, width, WINDOW):
        cut = slice(at, min(at + WINDOW, width))
        gate = lax.dot_general(act, wg[cut, :], NT, preferred_element_type=F32)
        up = lax.dot_general(act, wu[cut, :], NT, preferred_element_type=F32)
        inner = (jax.nn.gelu(gate, approximate=True) * up).astype(BF16)
        down = jnp.dot(inner, wd[cut, :], preferred_element_type=F32)
        if at == 0:
            part[...] = down
        else:
            part[...] += down
    swap.wait_send()
    mate_sum(part, half_ref, got, ssem, rsem, core, mate)


def feed(layer, heads, hid, ln, weights, cid):
    rows, dim = hid.shape
    width = weights[1].shape[1]
    own, inner = heads.shape
    return pl.pallas_call(
        functools.partial(feed_kernel, layer),
        out_shape=[jax.ShapeDtypeStruct((rows, dim), F32), jax.ShapeDtypeStruct((own, dim), F32)],
        in_specs=[vspec()] * 3 + [aspec()] * 4,
        out_specs=[vspec()] * 2,
        scratch_shapes=[pltpu.VMEM((inner, dim), BF16)] + [pltpu.VMEM((width, dim), BF16)] * 3 + [
            pltpu.VMEM((2, own, inner), F32), pltpu.VMEM((rows, dim), F32), pltpu.VMEM((own, dim), F32),
            pltpu.SemaphoreType.DMA((4,))] + [pltpu.SemaphoreType.DMA] * 4,
        compiler_params=pltpu.CompilerParams(collective_id=cid, has_side_effects=True, vmem_limit_bytes=40 * MIB),
        name=f"feed{layer}",
    )(heads, hid, ln, *weights)


def attend_kernel(layer, steps, normalizer, *refs):
    core_ref, start_ref, startv_ref, cos_ref, sin_ref, ln_ref, qk_ref, ar_ref, *refs = refs
    if layer == 0:
        wq_hbm, wk_hbm, wv_hbm, k_hbm, v_hbm, *refs = refs
    else:
        prev_ref, wq_hbm, wk_hbm, wv_hbm, k_hbm, v_hbm, _, _, *refs = refs
    hid_ref, heads_ref, fresh_hbm, ko_hbm, vo_hbm, wq, wk, wv, qs, fresh, os, wsem, fsem, kbuf, vbuf, rsem, osem = refs
    heads = wq.shape[1] // HEAD
    half = qs.shape[1] // TILE
    nblk = half // NB
    hrows = half * steps
    core = core_ref[0]
    ln = lambda l, j: ln_ref[4 * l + j:4 * l + j + 1, :]
    weights = [(wq_hbm, wq), (wk_hbm, wk), (wv_hbm, wv)]
    wcopies = [pltpu.make_async_copy(src.at[layer], dst, wsem.at[n]) for n, (src, dst) in enumerate(weights)]
    stream = Stream(layer, core * half, (k_hbm, v_hbm), (ko_hbm, vo_hbm), (kbuf, vbuf), rsem, osem)
    for c in wcopies:
        c.start()
    stream.begin(0, 2)

    if layer == 0:
        hid = ar_ref[...] * normalizer
    else:
        hid = prev_ref[...] + rms(ar_ref[...], ln(layer - 1, 3))
    hid_ref[...] = hid
    qs[...] = jnp.zeros_like(qs)
    fresh[...] = jnp.zeros_like(fresh)
    act = rms(hid, ln(layer, 0)).astype(BF16)
    for c in wcopies:
        c.wait()
    stream.begin(2, NBUF)

    def roped(x, weight, at):
        x = rms(x, weight)
        a, b = x[:, :LANES], x[:, LANES:]
        c, s = cos_ref[at, :], sin_ref[at, :]
        return a * c - b * s, b * c + a * s

    def put_fresh(kv, pair):
        for c in range(2):
            for t in range(steps):
                r = c * hrows + t * half
                for g in range(2):
                    fresh[2 * kv + g, pl.ds(c * half * TILE + t, half, stride=TILE), :] = pair[g][r:r + half, :]

    k = jnp.dot(act, wk[...], preferred_element_type=F32)
    put_fresh(0, roped(k, qk_ref[2 * layer + 1:2 * layer + 2, :], slice(None)))
    v = jnp.dot(act, wv[...], preferred_element_type=F32)
    put_fresh(1, (v[:, :LANES], v[:, LANES:]))
    away = pl.ds(pl.multiple_of((1 - core) * half * TILE, TILE), half * TILE)
    keep = pltpu.make_async_copy(fresh.at[:, away, :], fresh_hbm, fsem)

    mine = pl.ds(pl.multiple_of(core * hrows, 8), hrows)
    own = rms(hid_ref[mine, :], ln(layer, 0)).astype(BF16)
    for h in range(heads):
        q = jnp.dot(own, wq[:, h * HEAD:(h + 1) * HEAD], preferred_element_type=F32)
        pair = roped(q, qk_ref[2 * layer:2 * layer + 1, :], mine)
        for g in range(2):
            for t in range(steps):
                qs[g, pl.ds(t * heads + h, half, stride=TILE), :] = pair[g][t * half:(t + 1) * half, :]

    scale = HEAD ** -0.5
    m_rows = NB * TILE

    def body(i, slot):
        at = tiles(i)
        gat = tiles(core * nblk + i)
        qb = wide(qs, 0, at).astype(BF16)
        kf = wide(fresh, 0, gat)
        vf = wide(fresh, 2, gat)
        start = startv_ref[gat, :]
        row = lax.broadcasted_iota(jnp.int32, (m_rows, LANES), 0)
        lane = lax.broadcasted_iota(jnp.int32, (m_rows, LANES), 1)
        t = lax.shift_right_logical(row & (TILE - 1), 2)
        old = jnp.concatenate([lax.dot_general(qb[TILE * j:TILE * (j + 1), :], kbuf[slot, j], NT, preferred_element_type=F32) for j in range(NB)], axis=0) * scale
        new = lax.dot_general(qb, kf.astype(BF16), NT, preferred_element_type=F32) * scale
        cols = []
        for g in range(0, WINDOW, LANES):
            s = lane + g
            ok = (s <= start + t) & (((s - start) & (WINDOW - 1)) > t)
            cols.append(jnp.where(ok, old[:, g:g + LANES], NEG))
        ok = (row - (row & (TILE - 1)) == lane - (lane & (TILE - 1))) & ((lane & (TILE - 1)) <= t)
        cols.append(jnp.where(ok, new, NEG))
        top = functools.reduce(jnp.maximum, cols)
        top = jnp.max(top, axis=-1, keepdims=True)
        exps = [jnp.exp(c - top) for c in cols]
        tot = jnp.sum(functools.reduce(jnp.add, exps), axis=-1, keepdims=True)
        inv = 1.0 / tot
        pold = jnp.concatenate([(e * inv).astype(BF16) for e in exps[:-1]], axis=1)
        pnew = (exps[-1] * inv).astype(BF16)
        out = jnp.dot(pnew, vf.astype(BF16), preferred_element_type=F32)
        out = out + jnp.concatenate([jnp.dot(pold[TILE * j:TILE * (j + 1), :], vbuf[slot, j], preferred_element_type=F32) for j in range(NB)], axis=0)
        os[0, at, :] = out[:, :LANES]
        os[1, at, :] = out[:, LANES:]
        stream.change(i, slot, start_ref, (kf, vf), steps)

    keep.start()
    stream.run(nblk, body)
    for h in range(heads):
        for g in range(2):
            for t in range(steps):
                value = os[g, pl.ds(t * heads + h, half, stride=TILE), :].astype(BF16).astype(F32)
                col = h * HEAD + g * LANES
                heads_ref[t * half:(t + 1) * half, col:col + LANES] = value
    keep.wait()
    stream.end(nblk)


def attend(layer, small, ar, prev, weights, caches, outs):
    batch = caches[0].shape[1]
    rows, dim = ar.shape
    half = batch // 2
    inner = weights[0].shape[2]
    normalizer = float(np.float32(dim ** 0.5).astype(BF16))
    ins = list(small) + [ar] + ([] if prev is None else [prev]) + list(weights) + list(caches)
    specs = [sspec()] * 2 + [vspec()] * (len(ins) - 7) + [aspec()] * 5
    alias = {}
    if outs is not None:
        alias = {len(ins): 3, len(ins) + 1: 4}
        ins += list(outs)
        specs += [aspec()] * 2
    return pl.pallas_call(
        functools.partial(attend_kernel, layer, rows // batch, normalizer),
        out_shape=[jax.ShapeDtypeStruct((rows, dim), F32), jax.ShapeDtypeStruct((rows // 2, inner), F32),
                   jax.ShapeDtypeStruct((4, half * TILE, LANES), F32)] + cache_shapes(caches),
        in_specs=specs,
        out_specs=[vspec(), vspec()] + [aspec()] * 3,
        scratch_shapes=[
            pltpu.VMEM((dim, inner), BF16), pltpu.VMEM((dim, HEAD), BF16), pltpu.VMEM((dim, HEAD), BF16),
            pltpu.VMEM((2, half * TILE, LANES), F32), pltpu.VMEM((4, batch * TILE, LANES), F32), pltpu.VMEM((2, half * TILE, LANES), F32),
            pltpu.SemaphoreType.DMA((3,)), pltpu.SemaphoreType.DMA,
        ] + stream_scratch(),
        input_output_aliases=alias,
        compiler_params=pltpu.CompilerParams(vmem_limit_bytes=42 * MIB),
        name=f"attend{layer}",
    )(*ins)


TV = 1024
EBUF = 8
PIECES = 2


def scores_kernel(nblk, ar_ref, prev_ref, ln_ref, nf_ref, tgt_ref, e_hbm, out_ref, f_ref, ebuf, za, zb, m_ref, s_ref, t_ref, sem):
    rows, dim = f_ref.shape

    cut = TV // PIECES

    def fetch(i, slot):
        return [pltpu.make_async_copy(e_hbm.at[pl.ds(pl.multiple_of(i * TV + n * cut, cut), cut), :],
                                      ebuf.at[slot, pl.ds(n * cut, cut), :], sem.at[slot, n]) for n in range(PIECES)]

    def fetch_start(i, slot):
        for n, c in enumerate(fetch(i, slot)):
            c.start(priority=n % 2)

    def fetch_wait(i, slot):
        for c in fetch(i, slot):
            c.wait()

    for i in range(EBUF - 2):
        fetch_start(i, i)
    hid = prev_ref[...] + rms(ar_ref[...], ln_ref[7:8, :])
    f_ref[...] = rms(hid, nf_ref[...]).astype(BF16)
    m_ref[...] = jnp.full_like(m_ref, -jnp.inf)
    s_ref[...] = jnp.zeros_like(s_ref)
    t_ref[...] = jnp.zeros_like(t_ref)

    def dots(slot, z):
        for c in range(TV // 256):
            z[:, c * 256:(c + 1) * 256] = lax.dot_general(f_ref[...], ebuf[slot, c * 256:(c + 1) * 256, :], NT, preferred_element_type=F32)

    def fold(i, z):
        for r in range(rows // 8):
            sl = slice(r * 8, (r + 1) * 8)
            vals = [z[sl, g * 128:(g + 1) * 128] for g in range(TV // 128)]
            top = m_ref[sl, :]
            tops = list(vals)
            while len(tops) > 1:
                tops = [jnp.maximum(tops[n], tops[n + 1]) for n in range(0, len(tops), 2)]
            new = jnp.maximum(top, tops[0])
            m_ref[sl, :] = new
            exps = [jnp.exp(v - new) for v in vals]
            while len(exps) > 1:
                exps = [exps[n] + exps[n + 1] for n in range(0, len(exps), 2)]
            s_ref[sl, :] = s_ref[sl, :] * jnp.exp(top - new) + exps[0]
            want = tgt_ref[sl, :]
            hit = t_ref[sl, :]
            for g, v in enumerate(vals):
                hit = jnp.where(want == i * TV + g * 128, v, hit)
            t_ref[sl, :] = hit

    def prep(i, slot):
        fetch_wait(i, slot)

    def more(i):
        @pl.when(i < nblk)
        def _():
            fetch_start(i, lax.rem(i, EBUF))

    fetch_wait(0, 0)
    more(EBUF - 2)
    dots(0, za)

    def pair(n, carry):
        a = 2 * n + 1
        b = a + 1
        prep(a, lax.rem(a, EBUF))
        prep(b, lax.rem(b, EBUF))
        more(a + EBUF - 2)
        more(b + EBUF - 2)
        dots(lax.rem(a, EBUF), zb)
        fold(a - 1, za)
        dots(lax.rem(b, EBUF), za)
        fold(a, zb)
        return carry

    lax.fori_loop(0, (nblk - 2) // 2, pair, 0)
    last = nblk - 1
    prep(last, last % EBUF)
    dots(last % EBUF, zb)
    fold(last - 1, za)
    fold(last, zb)

    m = m_ref[...]
    top = jnp.max(m, axis=-1, keepdims=True)
    tot = jnp.sum(s_ref[...] * jnp.exp(m - top), axis=-1, keepdims=True)
    tgt = jnp.sum(t_ref[...], axis=-1, keepdims=True)
    lane = lax.broadcasted_iota(jnp.int32, (rows, 128), 1)
    pack = jnp.where(lane == 0, top, jnp.where(lane == 1, tot, jnp.where(lane == 2, tgt, 0.0)))
    pad = out_ref.shape[1] - rows
    pack = jnp.concatenate([pack, jnp.zeros((pad, 128), F32)], axis=0)
    out_ref[...] = jnp.transpose(pack)[:8, :]


def table_scores(ar, prev, ln, nf, tgt, table):
    rows, dim = ar.shape
    nblk = table.shape[0] // TV
    lanes = -(-rows // 128) * 128
    return pl.pallas_call(
        functools.partial(scores_kernel, nblk),
        out_shape=jax.ShapeDtypeStruct((8, lanes), F32),
        in_specs=[vspec()] * 5 + [aspec()],
        out_specs=vspec(),
        scratch_shapes=[
            pltpu.VMEM((rows, dim), BF16), pltpu.VMEM((EBUF, TV, dim), BF16),
            pltpu.VMEM((rows, TV), F32), pltpu.VMEM((rows, TV), F32),
            pltpu.VMEM((rows, 128), F32), pltpu.VMEM((rows, 128), F32), pltpu.VMEM((rows, 128), F32),
            pltpu.SemaphoreType.DMA((EBUF, PIECES)),
        ],
        compiler_params=pltpu.CompilerParams(vmem_limit_bytes=32 * MIB),
        name="table_scores",
    )(ar, prev, ln, nf, tgt, table)


def combine_kernel(x_ref, out_ref, got, ssem, rsem):
    dp = lax.axis_index("dp")
    tp = lax.axis_index("tp")
    barrier = pltpu.get_barrier_semaphore()
    for d in range(1, 4):
        pl.semaphore_signal(barrier, inc=1, device_id=(dp, lax.rem(tp + d, 4)), device_id_type=MESH)
    pl.semaphore_wait(barrier, 3)
    sends = []
    for d in range(1, 4):
        sends.append(pltpu.make_async_remote_copy(src_ref=x_ref, dst_ref=got.at[d - 1], send_sem=ssem.at[d - 1], recv_sem=rsem.at[d - 1],
                                                  device_id=(dp, lax.rem(tp + d, 4)), device_id_type=MESH))
        sends[-1].start()
    for s in sends:
        s.wait()
    mine = x_ref[...]
    vals = [mine] + [got[d] for d in range(3)]
    ordered = []
    for dev in range(4):
        v = mine
        for d in range(1, 4):
            v = jnp.where(lax.rem(tp + 4 - d, 4) == dev, vals[d], v)
        ordered.append(v)
    top = jnp.maximum(jnp.maximum(ordered[0][0:1], ordered[1][0:1]), jnp.maximum(ordered[2][0:1], ordered[3][0:1]))
    tot = 0.0
    tgt = 0.0
    for v in ordered:
        tot = tot + v[1:2] * jnp.exp(v[0:1] - top)
        tgt = tgt + v[2:3]
    log_z = top + jnp.log(tot)
    lanes = out_ref.shape[1]
    row = lax.broadcasted_iota(jnp.int32, (8, lanes), 0)
    out_ref[...] = jnp.where(row == 0, tgt - log_z, log_z)


def combine(x, cid):
    return pl.pallas_call(
        combine_kernel,
        out_shape=jax.ShapeDtypeStruct(x.shape, F32),
        in_specs=[vspec()],
        out_specs=vspec(),
        scratch_shapes=[pltpu.VMEM((3,) + x.shape, F32), pltpu.SemaphoreType.DMA((3,)), pltpu.SemaphoreType.DMA((3,))],
        compiler_params=pltpu.CompilerParams(collective_id=cid, has_side_effects=True),
        name="combine_tp",
    )(x)


def solution(mesh):
    arg_specs = (P('dp', None), P('dp', None), P('dp'), P('tp', None), P(), P(), P(), P(), P(), P(), P(None, None, 'tp'), P(None, None, 'tp'), P(None, 'tp', None), P(), P(None, 'dp'), P(None, 'dp'))
    result_specs = (P('dp', None), P('dp', None), P(None, 'dp'), P(None, 'dp'))

    def decode_local(tokens, targets, start_pos, embed_table, layer_norms, w_q, w_k, w_v, qk_norms, w_o, w_gate, w_up, w_down, norm_final, k_cache, v_cache):
        batch, steps = tokens.shape
        layers, dim, heads, head_dim = w_q.shape
        window = k_cache.shape[2]
        vocab_local = embed_table.shape[0]
        rows = batch * steps
        vocab_start = lax.axis_index('tp') * vocab_local
        def by_row(x):
            return jnp.swapaxes(x.reshape(2, batch // 2, steps), 1, 2).reshape(rows)

        def from_row(x):
            return jnp.swapaxes(x.reshape(2, steps, batch // 2), 1, 2).reshape(batch, steps)

        core = (lax.axis_index('tp') % 2).reshape(1)
        positions = by_row(start_pos[:, None] + jnp.arange(steps)[None, :])
        inv_freq = ROPE_BASE ** (-2.0 * jnp.arange(head_dim // 2, dtype=F32) / head_dim)
        angles = positions.astype(F32)[:, None] * inv_freq[None, :]
        startv = jnp.broadcast_to(start_pos[:, None, None], (batch, 16, 128)).reshape(batch * 16, 128)
        ln = layer_norms.reshape(layers * 4, dim)
        small = (core, start_pos, startv, jnp.cos(angles), jnp.sin(angles), ln, qk_norms.reshape(layers * 2, head_dim))
        qkv = (w_q.reshape(layers, dim, heads * head_dim), w_k.reshape(layers, dim, head_dim), w_v.reshape(layers, dim, head_dim))
        ffn = (w_o.reshape(layers, heads * head_dim, dim), jnp.swapaxes(w_gate, 1, 2), jnp.swapaxes(w_up, 1, 2), w_down)
        caches = (k_cache.reshape(layers, batch, window, head_dim), v_cache.reshape(layers, batch, window, head_dim))
        ar = share(pair_sum(gather_rows(by_row(tokens) - vocab_start, embed_table), 0), 1)
        hid, outs = None, None
        for layer in range(layers):
            hid, own_heads, fresh, *outs = attend(layer, small, ar, hid, qkv, caches, outs)
            hid, half = feed(layer, own_heads, hid, ln, ffn, 2 + layer)
            outs = carry_other(layer, steps, core, start_pos, fresh, caches, outs)
            ar = share(half, 4 + layer)
        tgt = (by_row(targets) - vocab_start)[:, None] - jnp.arange(LANES)[None, :]
        stats = table_scores(ar, hid, ln, norm_final.reshape(1, dim), tgt, embed_table)
        res = combine(stats, 4 + layers)
        return from_row(res[0, :rows]), from_row(res[1, :rows]), outs[0].reshape(k_cache.shape), outs[1].reshape(v_cache.shape)

    return jax.shard_map(decode_local, mesh=mesh, in_specs=arg_specs, out_specs=result_specs, check_vma=False)
```

```python
import functools

import jax
import jax.numpy as jnp
import numpy as np
from jax import lax
from jax.experimental import pallas as pl
from jax.experimental.pallas import tpu as pltpu
from jax.sharding import PartitionSpec as P

EPSILON = 1e-6
ROPE_BASE = 10000.0
NEG = -1e30
MESH = pl.DeviceIdType.MESH
F32 = jnp.float32
BF16 = jnp.bfloat16
NT = (((1,), (1,)), ((), ()))


def rms(values, weight):
    mean_sq = jnp.mean(values * values, axis=-1, keepdims=True)
    return values * lax.rsqrt(mean_sq + EPSILON) * (1.0 + weight)


def vspec():
    return pl.BlockSpec(memory_space=pltpu.VMEM)


def aspec():
    return pl.BlockSpec(memory_space=pl.ANY)


def sspec():
    return pl.BlockSpec(memory_space=pltpu.SMEM)


def gather_kernel(rows, grp_ref, col_ref, table_ref, out_ref, xbuf, sem):
    def issue(i, carry):
        src = pl.multiple_of(grp_ref[i] * 8, 8)
        dst = pl.multiple_of(i * 8, 8)
        pltpu.make_async_copy(table_ref.at[pl.ds(src, 8), :], xbuf.at[pl.ds(dst, 8), :], sem).start()
        return carry

    lax.fori_loop(0, rows, issue, 0, unroll=8)
    pltpu.make_async_copy(table_ref.at[pl.ds(0, rows * 8), :], xbuf, sem).wait()
    for c in range(rows // 32):
        lanes = lax.broadcasted_iota(jnp.int32, (32, 256), 1)
        pick = jnp.where(lanes == col_ref[c * 32:(c + 1) * 32, :], 1.0, 0.0).astype(BF16)
        out_ref[c * 32:(c + 1) * 32, :] = jnp.dot(pick, xbuf[c * 256:(c + 1) * 256, :], preferred_element_type=F32)


def gather_rows(ids, table):
    rows = ids.shape[0]
    vocab_local, dim = table.shape
    here = (ids >= 0) & (ids < vocab_local)
    safe = ids % vocab_local
    col = jnp.where(here, (jnp.arange(rows) % 32) * 8 + safe % 8, -1)[:, None]
    return pl.pallas_call(
        functools.partial(gather_kernel, rows),
        out_shape=jax.ShapeDtypeStruct((rows, dim), F32),
        in_specs=[sspec(), vspec(), aspec()],
        out_specs=vspec(),
        scratch_shapes=[pltpu.VMEM((rows * 8, dim), BF16), pltpu.SemaphoreType.DMA],
        compiler_params=pltpu.CompilerParams(vmem_limit_bytes=24 * 1024 * 1024),
        name="token_rows",
    )(safe // 8, col, table)


LANES = 128
HEAD = 2 * LANES
TILE = 16
WINDOW = 512
MIB = 1024 * 1024


def mate_of():
    tp = lax.axis_index("tp")
    core = lax.rem(tp, 2)
    return core, (lax.axis_index("dp"), tp + 1 - 2 * core)


def meet(mate):
    barrier = pltpu.get_barrier_semaphore()
    pl.semaphore_signal(barrier, inc=1, device_id=mate, device_id_type=MESH)
    pl.semaphore_wait(barrier, 1)


def send(src, dst, ssem, rsem, peer):
    return pltpu.make_async_remote_copy(src_ref=src, dst_ref=dst, send_sem=ssem, recv_sem=rsem, device_id=peer, device_id_type=MESH)


def part_rows(which, ref):
    hrows = ref.shape[0] // 2
    return pl.ds(pl.multiple_of(which * hrows, 8), hrows)


def mate_sum(part_ref, out_ref, got, ssem, rsem, core, mate):
    swap = send(part_ref.at[part_rows(1 - core, part_ref), :], got, ssem, rsem, mate)
    swap.start()
    swap.wait()
    out_ref[...] = part_ref[part_rows(core, part_ref), :] + got[...]


def pair_sum_kernel(part_ref, out_ref, got, ssem, rsem):
    core, mate = mate_of()
    meet(mate)
    mate_sum(part_ref, out_ref, got, ssem, rsem, core, mate)


def pair_share_kernel(a_ref, b_ref, out_ref, total, got, ssem, rsem):
    core, mate = mate_of()
    total[...] = a_ref[...] + b_ref[...]
    meet(mate)
    swap = send(total, got, ssem, rsem, mate)
    swap.start()
    out_ref[part_rows(core, out_ref), :] = total[...]
    swap.wait()
    out_ref[part_rows(1 - core, out_ref), :] = got[...]


def pair_call(kernel, out_rows, ins, scratch, cid, name):
    dim = ins[0].shape[1]
    return pl.pallas_call(
        kernel,
        out_shape=jax.ShapeDtypeStruct((out_rows, dim), F32),
        in_specs=[vspec()] * len(ins),
        out_specs=vspec(),
        scratch_shapes=[pltpu.VMEM(shape, F32) for shape in scratch] + [pltpu.SemaphoreType.DMA] * 2,
        compiler_params=pltpu.CompilerParams(collective_id=cid, has_side_effects=True, vmem_limit_bytes=12 * MIB),
        name=name,
    )(*ins)


def pair_sum(part, cid):
    rows, dim = part.shape
    return pair_call(pair_sum_kernel, rows // 2, [part], [(rows // 2, dim)], cid, "pair_sum")


def share(half, cid):
    far = lax.ppermute(half, 'tp', [(n, (n + 2) % 4) for n in range(4)])
    return pair_call(pair_share_kernel, half.shape[0] * 2, [half, far], [half.shape] * 2, cid, "pair_share")


NB = 8
NBUF = 4


class Stream:
    def __init__(self, layer, base, sources, targets, bufs, rsem, osem):
        self.layer, self.base = layer, base
        self.sources, self.targets, self.bufs, self.rsem, self.osem = sources, targets, bufs, rsem, osem

    def rows(self, i):
        return pl.ds(pl.multiple_of(self.base + i * NB, NB), NB)

    def reads(self, i, slot):
        return [pltpu.make_async_copy(src.at[self.layer, self.rows(i)], buf.at[slot], self.rsem.at[n, slot])
                for n, (src, buf) in enumerate(zip(self.sources, self.bufs))]

    def writes(self, i, slot):
        return [pltpu.make_async_copy(buf.at[slot], dst.at[self.layer, self.rows(i)], self.osem.at[n, slot])
                for n, (dst, buf) in enumerate(zip(self.targets, self.bufs))]

    def begin(self, first, last):
        for i in range(first, last):
            for c in self.reads(i, i):
                c.start()

    def run(self, nblk, body):
        def block(i, carry):
            slot = lax.rem(i, NBUF)
            for c in self.reads(i, slot):
                c.wait()

            @pl.when(i >= 1)
            def _():
                for c in self.writes(i - 1, lax.rem(i + NBUF - 1, NBUF)):
                    c.start()

            @pl.when(i >= 2)
            def _():
                for c in self.writes(i - 2, lax.rem(i + NBUF - 2, NBUF)):
                    c.wait()

            @pl.when((i + 2 >= NBUF) & (i + 2 < nblk))
            def _():
                for c in self.reads(i + 2, lax.rem(i + 2, NBUF)):
                    c.start()

            body(i, slot)
            return carry

        lax.fori_loop(0, nblk, block, 0)
        for c in self.writes(nblk - 1, (nblk - 1) % NBUF):
            c.start()

    def end(self, nblk):
        for i in (nblk - 2, nblk - 1):
            for c in self.writes(i, i % NBUF):
                c.wait()

    def change(self, i, slot, start_ref, fresh, steps):
        sub = lax.broadcasted_iota(jnp.int32, (TILE, HEAD), 0)
        for first in (0, NB // 2):
            pending = []
            for j in range(first, first + NB // 2):
                st = start_ref[self.base + i * NB + j]
                for s in (st & (WINDOW - 1), (st + steps - 1) & (WINDOW - 1)):
                    at = pl.multiple_of(s - (s & (TILE - 1)), TILE)
                    dist = (sub + at - st) & (WINDOW - 1)
                    for buf, new in zip(self.bufs, fresh):
                        value = buf[slot, j, pl.ds(at, TILE), :].astype(F32)
                        for t in range(steps):
                            value = jnp.where(dist == t, new[TILE * j + t:TILE * j + t + 1, :], value)
                        pending.append((buf, j, at, value.astype(BF16)))
            for buf, j, at, value in pending:
                buf[slot, j, pl.ds(at, TILE), :] = value


def stream_scratch():
    buf = pltpu.VMEM((NBUF, NB, WINDOW, HEAD), BF16)
    sem = pltpu.SemaphoreType.DMA((2, NBUF))
    return [buf, buf, sem, sem]


def cache_shapes(caches):
    return [jax.ShapeDtypeStruct(c.shape, c.dtype) for c in caches]


def wide(ref, n, at):
    return jnp.concatenate([ref[n, at, :], ref[n + 1, at, :]], axis=1)


def tiles(i):
    return pl.ds(pl.multiple_of(i * NB * TILE, NB * TILE), NB * TILE)


def carry_kernel(layer, steps, core_ref, start_ref, fresh, k_hbm, v_hbm, _k, _v, ko_hbm, vo_hbm, kbuf, vbuf, rsem, osem):
    half = fresh.shape[1] // TILE
    nblk = half // NB
    stream = Stream(layer, (1 - core_ref[0]) * half, (k_hbm, v_hbm), (ko_hbm, vo_hbm), (kbuf, vbuf), rsem, osem)
    stream.begin(0, NBUF)
    stream.run(nblk, lambda i, slot: stream.change(i, slot, start_ref, (wide(fresh, 0, tiles(i)), wide(fresh, 2, tiles(i))), steps))
    stream.end(nblk)


def carry_other(layer, steps, core, start, fresh, caches, outs):
    return pl.pallas_call(
        functools.partial(carry_kernel, layer, steps),
        out_shape=cache_shapes(caches),
        in_specs=[sspec(), sspec(), vspec()] + [aspec()] * 4,
        out_specs=[aspec()] * 2,
        scratch_shapes=stream_scratch(),
        input_output_aliases={5: 0, 6: 1},
        compiler_params=pltpu.CompilerParams(vmem_limit_bytes=24 * MIB),
        cost_estimate=pl.CostEstimate(flops=10 ** 10, bytes_accessed=48 * MIB, transcendentals=0),
        name=f"carry{layer}",
    )(core, start, fresh, *caches, *outs)


def feed_kernel(layer, heads_ref, hid_ref, ln_ref, wo_hbm, wg_hbm, wu_hbm, wd_hbm,
                hid_out, half_ref, wo, wg, wu, wd, both, part, got, wsem, hsend, hrecv, ssem, rsem):
    core, mate = mate_of()
    weights = [(wo_hbm, wo), (wg_hbm, wg), (wu_hbm, wu), (wd_hbm, wd)]
    wcopies = [pltpu.make_async_copy(src.at[layer], dst, wsem.at[n]) for n, (src, dst) in enumerate(weights)]
    for c in wcopies:
        c.start()
    meet(mate)
    swap = send(heads_ref, both.at[core], hsend, hrecv, mate)
    swap.start()
    both[core] = heads_ref[...]
    ln = lambda j: ln_ref[4 * layer + j:4 * layer + j + 1, :]
    wcopies[0].wait()
    swap.wait_recv()
    x = jnp.concatenate([both[0], both[1]], axis=0).astype(BF16)
    hid = hid_ref[...] + rms(jnp.dot(x, wo[...], preferred_element_type=F32), ln(1))
    hid_out[...] = hid
    act = rms(hid, ln(2)).astype(BF16)
    for c in wcopies[1:3]:
        c.wait()
    width = wg.shape[0]
    for at in range(0, width, WINDOW):
        cut = slice(at, min(at + WINDOW, width))
        gate = lax.dot_general(act, wg[cut, :], NT, preferred_element_type=F32)
        up = lax.dot_general(act, wu[cut, :], NT, preferred_element_type=F32)
        inner = (jax.nn.gelu(gate, approximate=True) * up).astype(BF16)
        if at == 0:
            wcopies[3].wait()
        down = jnp.dot(inner, wd[cut, :], preferred_element_type=F32)
        if at == 0:
            part[...] = down
        else:
            part[...] += down
    swap.wait_send()
    mate_sum(part, half_ref, got, ssem, rsem, core, mate)


def feed(layer, heads, hid, ln, weights, cid):
    rows, dim = hid.shape
    width = weights[1].shape[1]
    own, inner = heads.shape
    return pl.pallas_call(
        functools.partial(feed_kernel, layer),
        out_shape=[jax.ShapeDtypeStruct((rows, dim), F32), jax.ShapeDtypeStruct((own, dim), F32)],
        in_specs=[vspec()] * 3 + [aspec()] * 4,
        out_specs=[vspec()] * 2,
        scratch_shapes=[pltpu.VMEM((inner, dim), BF16)] + [pltpu.VMEM((width, dim), BF16)] * 3 + [
            pltpu.VMEM((2, own, inner), F32), pltpu.VMEM((rows, dim), F32), pltpu.VMEM((own, dim), F32),
            pltpu.SemaphoreType.DMA((4,))] + [pltpu.SemaphoreType.DMA] * 4,
        compiler_params=pltpu.CompilerParams(collective_id=cid, has_side_effects=True, vmem_limit_bytes=40 * MIB),
        name=f"feed{layer}",
    )(heads, hid, ln, *weights)


def attend_kernel(layer, steps, normalizer, *refs):
    core_ref, start_ref, startv_ref, cos_ref, sin_ref, ln_ref, qk_ref, ar_ref, *refs = refs
    if layer == 0:
        wq_hbm, wk_hbm, wv_hbm, k_hbm, v_hbm, *refs = refs
    else:
        prev_ref, wq_hbm, wk_hbm, wv_hbm, k_hbm, v_hbm, _, _, *refs = refs
    hid_ref, heads_ref, fresh_hbm, ko_hbm, vo_hbm, wq, wk, wv, qs, fresh, os, wsem, fsem, kbuf, vbuf, rsem, osem = refs
    heads = wq.shape[1] // HEAD
    half = qs.shape[1] // TILE
    nblk = half // NB
    hrows = half * steps
    core = core_ref[0]
    ln = lambda l, j: ln_ref[4 * l + j:4 * l + j + 1, :]
    weights = [(wq_hbm, wq), (wk_hbm, wk), (wv_hbm, wv)]
    wcopies = [pltpu.make_async_copy(src.at[layer], dst, wsem.at[n]) for n, (src, dst) in enumerate(weights)]
    stream = Stream(layer, core * half, (k_hbm, v_hbm), (ko_hbm, vo_hbm), (kbuf, vbuf), rsem, osem)
    for c in wcopies:
        c.start()
    stream.begin(0, 2)

    if layer == 0:
        hid = ar_ref[...] * normalizer
    else:
        hid = prev_ref[...] + rms(ar_ref[...], ln(layer - 1, 3))
    hid_ref[...] = hid
    qs[...] = jnp.zeros_like(qs)
    fresh[...] = jnp.zeros_like(fresh)
    act = rms(hid, ln(layer, 0)).astype(BF16)
    for c in wcopies:
        c.wait()
    stream.begin(2, NBUF)

    def roped(x, weight, at):
        x = rms(x, weight)
        a, b = x[:, :LANES], x[:, LANES:]
        c, s = cos_ref[at, :], sin_ref[at, :]
        return a * c - b * s, b * c + a * s

    def put_fresh(kv, pair):
        for c in range(2):
            for t in range(steps):
                r = c * hrows + t * half
                for g in range(2):
                    fresh[2 * kv + g, pl.ds(c * half * TILE + t, half, stride=TILE), :] = pair[g][r:r + half, :]

    k = jnp.dot(act, wk[...], preferred_element_type=F32)
    put_fresh(0, roped(k, qk_ref[2 * layer + 1:2 * layer + 2, :], slice(None)))
    v = jnp.dot(act, wv[...], preferred_element_type=F32)
    put_fresh(1, (v[:, :LANES], v[:, LANES:]))
    away = pl.ds(pl.multiple_of((1 - core) * half * TILE, TILE), half * TILE)
    keep = pltpu.make_async_copy(fresh.at[:, away, :], fresh_hbm, fsem)

    mine = pl.ds(pl.multiple_of(core * hrows, 8), hrows)
    own = rms(hid_ref[mine, :], ln(layer, 0)).astype(BF16)
    for h in range(heads):
        q = jnp.dot(own, wq[:, h * HEAD:(h + 1) * HEAD], preferred_element_type=F32)
        pair = roped(q, qk_ref[2 * layer:2 * layer + 1, :], mine)
        for g in range(2):
            for t in range(steps):
                qs[g, pl.ds(t * heads + h, half, stride=TILE), :] = pair[g][t * half:(t + 1) * half, :]

    scale = HEAD ** -0.5
    m_rows = NB * TILE

    def body(i, slot):
        at = tiles(i)
        gat = tiles(core * nblk + i)
        qb = wide(qs, 0, at).astype(BF16)
        kf = wide(fresh, 0, gat)
        vf = wide(fresh, 2, gat)
        start = startv_ref[gat, :]
        row = lax.broadcasted_iota(jnp.int32, (m_rows, LANES), 0)
        lane = lax.broadcasted_iota(jnp.int32, (m_rows, LANES), 1)
        t = lax.shift_right_logical(row & (TILE - 1), 2)
        old = jnp.concatenate([lax.dot_general(qb[TILE * j:TILE * (j + 1), :], kbuf[slot, j], NT, preferred_element_type=F32) for j in range(NB)], axis=0) * scale
        new = lax.dot_general(qb, kf.astype(BF16), NT, preferred_element_type=F32) * scale
        cols = []
        for g in range(0, WINDOW, LANES):
            s = lane + g
            ok = (s <= start + t) & (((s - start) & (WINDOW - 1)) > t)
            cols.append(jnp.where(ok, old[:, g:g + LANES], NEG))
        ok = (row - (row & (TILE - 1)) == lane - (lane & (TILE - 1))) & ((lane & (TILE - 1)) <= t)
        cols.append(jnp.where(ok, new, NEG))
        top = functools.reduce(jnp.maximum, cols)
        top = jnp.max(top, axis=-1, keepdims=True)
        exps = [jnp.exp(c - top) for c in cols]
        tot = jnp.sum(functools.reduce(jnp.add, exps), axis=-1, keepdims=True)
        inv = 1.0 / tot
        pold = jnp.concatenate([(e * inv).astype(BF16) for e in exps[:-1]], axis=1)
        pnew = (exps[-1] * inv).astype(BF16)
        out = jnp.dot(pnew, vf.astype(BF16), preferred_element_type=F32)
        out = out + jnp.concatenate([jnp.dot(pold[TILE * j:TILE * (j + 1), :], vbuf[slot, j], preferred_element_type=F32) for j in range(NB)], axis=0)
        os[0, at, :] = out[:, :LANES]
        os[1, at, :] = out[:, LANES:]
        stream.change(i, slot, start_ref, (kf, vf), steps)

    keep.start()
    stream.run(nblk, body)
    for h in range(heads):
        for g in range(2):
            for t in range(steps):
                value = os[g, pl.ds(t * heads + h, half, stride=TILE), :].astype(BF16).astype(F32)
                col = h * HEAD + g * LANES
                heads_ref[t * half:(t + 1) * half, col:col + LANES] = value
    keep.wait()
    stream.end(nblk)


def attend(layer, small, ar, prev, weights, caches, outs):
    batch = caches[0].shape[1]
    rows, dim = ar.shape
    half = batch // 2
    inner = weights[0].shape[2]
    normalizer = float(np.float32(dim ** 0.5).astype(BF16))
    ins = list(small) + [ar] + ([] if prev is None else [prev]) + list(weights) + list(caches)
    specs = [sspec()] * 2 + [vspec()] * (len(ins) - 7) + [aspec()] * 5
    alias = {}
    if outs is not None:
        alias = {len(ins): 3, len(ins) + 1: 4}
        ins += list(outs)
        specs += [aspec()] * 2
    return pl.pallas_call(
        functools.partial(attend_kernel, layer, rows // batch, normalizer),
        out_shape=[jax.ShapeDtypeStruct((rows, dim), F32), jax.ShapeDtypeStruct((rows // 2, inner), F32),
                   jax.ShapeDtypeStruct((4, half * TILE, LANES), F32)] + cache_shapes(caches),
        in_specs=specs,
        out_specs=[vspec(), vspec()] + [aspec()] * 3,
        scratch_shapes=[
            pltpu.VMEM((dim, inner), BF16), pltpu.VMEM((dim, HEAD), BF16), pltpu.VMEM((dim, HEAD), BF16),
            pltpu.VMEM((2, half * TILE, LANES), F32), pltpu.VMEM((4, batch * TILE, LANES), F32), pltpu.VMEM((2, half * TILE, LANES), F32),
            pltpu.SemaphoreType.DMA((3,)), pltpu.SemaphoreType.DMA,
        ] + stream_scratch(),
        input_output_aliases=alias,
        compiler_params=pltpu.CompilerParams(vmem_limit_bytes=42 * MIB),
        name=f"attend{layer}",
    )(*ins)


TV = 1024
EBUF = 8
PIECES = 2


def scores_kernel(nblk, ar_ref, prev_ref, ln_ref, nf_ref, tgt_ref, e_hbm, out_ref, f_ref, ebuf, za, zb, m_ref, s_ref, t_ref, sem):
    rows, dim = f_ref.shape

    cut = TV // PIECES

    def fetch(i, slot):
        return [pltpu.make_async_copy(e_hbm.at[pl.ds(pl.multiple_of(i * TV + n * cut, cut), cut), :],
                                      ebuf.at[slot, pl.ds(n * cut, cut), :], sem.at[slot, n]) for n in range(PIECES)]

    def fetch_start(i, slot):
        for n, c in enumerate(fetch(i, slot)):
            c.start(priority=n % 2)

    def fetch_wait(i, slot):
        for c in fetch(i, slot):
            c.wait()

    for i in range(EBUF - 2):
        fetch_start(i, i)
    hid = prev_ref[...] + rms(ar_ref[...], ln_ref[7:8, :])
    f_ref[...] = rms(hid, nf_ref[...]).astype(BF16)
    m_ref[...] = jnp.full_like(m_ref, -jnp.inf)
    s_ref[...] = jnp.zeros_like(s_ref)
    t_ref[...] = jnp.zeros_like(t_ref)

    def dots(slot, z):
        for c in range(TV // 512):
            z[:, c * 512:(c + 1) * 512] = lax.dot_general(f_ref[...], ebuf[slot, c * 512:(c + 1) * 512, :], NT, preferred_element_type=F32)

    def fold(i, z):
        for r in range(rows // 8):
            sl = slice(r * 8, (r + 1) * 8)
            vals = [z[sl, g * 128:(g + 1) * 128] for g in range(TV // 128)]
            top = m_ref[sl, :]
            tops = list(vals)
            while len(tops) > 1:
                tops = [jnp.maximum(tops[n], tops[n + 1]) for n in range(0, len(tops), 2)]
            new = jnp.maximum(top, tops[0])
            m_ref[sl, :] = new
            exps = [jnp.exp(v - new) for v in vals]
            while len(exps) > 1:
                exps = [exps[n] + exps[n + 1] for n in range(0, len(exps), 2)]
            s_ref[sl, :] = s_ref[sl, :] * jnp.exp(top - new) + exps[0]
            want = tgt_ref[sl, :]
            hit = t_ref[sl, :]
            for g, v in enumerate(vals):
                hit = jnp.where(want == i * TV + g * 128, v, hit)
            t_ref[sl, :] = hit

    def prep(i, slot):
        fetch_wait(i, slot)

    def more(i):
        @pl.when(i < nblk)
        def _():
            fetch_start(i, lax.rem(i, EBUF))

    fetch_wait(0, 0)
    more(EBUF - 2)
    dots(0, za)

    def pair(n, carry):
        a = 2 * n + 1
        b = a + 1
        prep(a, lax.rem(a, EBUF))
        prep(b, lax.rem(b, EBUF))
        more(a + EBUF - 2)
        more(b + EBUF - 2)
        dots(lax.rem(a, EBUF), zb)
        fold(a - 1, za)
        dots(lax.rem(b, EBUF), za)
        fold(a, zb)
        return carry

    lax.fori_loop(0, (nblk - 2) // 2, pair, 0)
    last = nblk - 1
    prep(last, last % EBUF)
    dots(last % EBUF, zb)
    fold(last - 1, za)
    fold(last, zb)

    m = m_ref[...]
    top = jnp.max(m, axis=-1, keepdims=True)
    tot = jnp.sum(s_ref[...] * jnp.exp(m - top), axis=-1, keepdims=True)
    tgt = jnp.sum(t_ref[...], axis=-1, keepdims=True)
    lane = lax.broadcasted_iota(jnp.int32, (rows, 128), 1)
    pack = jnp.where(lane == 0, top, jnp.where(lane == 1, tot, jnp.where(lane == 2, tgt, 0.0)))
    pad = out_ref.shape[1] - rows
    pack = jnp.concatenate([pack, jnp.zeros((pad, 128), F32)], axis=0)
    out_ref[...] = jnp.transpose(pack)[:8, :]


def table_scores(ar, prev, ln, nf, tgt, table):
    rows, dim = ar.shape
    nblk = table.shape[0] // TV
    lanes = -(-rows // 128) * 128
    return pl.pallas_call(
        functools.partial(scores_kernel, nblk),
        out_shape=jax.ShapeDtypeStruct((8, lanes), F32),
        in_specs=[vspec()] * 5 + [aspec()],
        out_specs=vspec(),
        scratch_shapes=[
            pltpu.VMEM((rows, dim), BF16), pltpu.VMEM((EBUF, TV, dim), BF16),
            pltpu.VMEM((rows, TV), F32), pltpu.VMEM((rows, TV), F32),
            pltpu.VMEM((rows, 128), F32), pltpu.VMEM((rows, 128), F32), pltpu.VMEM((rows, 128), F32),
            pltpu.SemaphoreType.DMA((EBUF, PIECES)),
        ],
        compiler_params=pltpu.CompilerParams(vmem_limit_bytes=32 * MIB),
        name="table_scores",
    )(ar, prev, ln, nf, tgt, table)


def combine_kernel(x_ref, out_ref, got, ssem, rsem):
    dp = lax.axis_index("dp")
    tp = lax.axis_index("tp")
    barrier = pltpu.get_barrier_semaphore()
    for d in range(1, 4):
        pl.semaphore_signal(barrier, inc=1, device_id=(dp, lax.rem(tp + d, 4)), device_id_type=MESH)
    pl.semaphore_wait(barrier, 3)
    sends = []
    for d in range(1, 4):
        sends.append(pltpu.make_async_remote_copy(src_ref=x_ref, dst_ref=got.at[d - 1], send_sem=ssem.at[d - 1], recv_sem=rsem.at[d - 1],
                                                  device_id=(dp, lax.rem(tp + d, 4)), device_id_type=MESH))
        sends[-1].start()
    for s in sends:
        s.wait()
    mine = x_ref[...]
    vals = [mine] + [got[d] for d in range(3)]
    ordered = []
    for dev in range(4):
        v = mine
        for d in range(1, 4):
            v = jnp.where(lax.rem(tp + 4 - d, 4) == dev, vals[d], v)
        ordered.append(v)
    top = jnp.maximum(jnp.maximum(ordered[0][0:1], ordered[1][0:1]), jnp.maximum(ordered[2][0:1], ordered[3][0:1]))
    tot = 0.0
    tgt = 0.0
    for v in ordered:
        tot = tot + v[1:2] * jnp.exp(v[0:1] - top)
        tgt = tgt + v[2:3]
    log_z = top + jnp.log(tot)
    lanes = out_ref.shape[1]
    row = lax.broadcasted_iota(jnp.int32, (8, lanes), 0)
    out_ref[...] = jnp.where(row == 0, tgt - log_z, log_z)


def combine(x, cid):
    return pl.pallas_call(
        combine_kernel,
        out_shape=jax.ShapeDtypeStruct(x.shape, F32),
        in_specs=[vspec()],
        out_specs=vspec(),
        scratch_shapes=[pltpu.VMEM((3,) + x.shape, F32), pltpu.SemaphoreType.DMA((3,)), pltpu.SemaphoreType.DMA((3,))],
        compiler_params=pltpu.CompilerParams(collective_id=cid, has_side_effects=True),
        name="combine_tp",
    )(x)


def solution(mesh):
    arg_specs = (P('dp', None), P('dp', None), P('dp'), P('tp', None), P(), P(), P(), P(), P(), P(), P(None, None, 'tp'), P(None, None, 'tp'), P(None, 'tp', None), P(), P(None, 'dp'), P(None, 'dp'))
    result_specs = (P('dp', None), P('dp', None), P(None, 'dp'), P(None, 'dp'))

    def decode_local(tokens, targets, start_pos, embed_table, layer_norms, w_q, w_k, w_v, qk_norms, w_o, w_gate, w_up, w_down, norm_final, k_cache, v_cache):
        batch, steps = tokens.shape
        layers, dim, heads, head_dim = w_q.shape
        window = k_cache.shape[2]
        vocab_local = embed_table.shape[0]
        rows = batch * steps
        vocab_start = lax.axis_index('tp') * vocab_local
        def by_row(x):
            return jnp.swapaxes(x.reshape(2, batch // 2, steps), 1, 2).reshape(rows)

        def from_row(x):
            return jnp.swapaxes(x.reshape(2, steps, batch // 2), 1, 2).reshape(batch, steps)

        core = (lax.axis_index('tp') % 2).reshape(1)
        positions = by_row(start_pos[:, None] + jnp.arange(steps)[None, :])
        inv_freq = ROPE_BASE ** (-2.0 * jnp.arange(head_dim // 2, dtype=F32) / head_dim)
        angles = positions.astype(F32)[:, None] * inv_freq[None, :]
        startv = jnp.broadcast_to(start_pos[:, None, None], (batch, 16, 128)).reshape(batch * 16, 128)
        ln = layer_norms.reshape(layers * 4, dim)
        small = (core, start_pos, startv, jnp.cos(angles), jnp.sin(angles), ln, qk_norms.reshape(layers * 2, head_dim))
        qkv = (w_q.reshape(layers, dim, heads * head_dim), w_k.reshape(layers, dim, head_dim), w_v.reshape(layers, dim, head_dim))
        ffn = (w_o.reshape(layers, heads * head_dim, dim), jnp.swapaxes(w_gate, 1, 2), jnp.swapaxes(w_up, 1, 2), w_down)
        caches = (k_cache.reshape(layers, batch, window, head_dim), v_cache.reshape(layers, batch, window, head_dim))
        ar = share(pair_sum(gather_rows(by_row(tokens) - vocab_start, embed_table), 0), 1)
        hid, outs = None, None
        for layer in range(layers):
            hid, own_heads, fresh, *outs = attend(layer, small, ar, hid, qkv, caches, outs)
            hid, half = feed(layer, own_heads, hid, ln, ffn, 2 + layer)
            outs = carry_other(layer, steps, core, start_pos, fresh, caches, outs)
            ar = share(half, 4 + layer)
        tgt = (by_row(targets) - vocab_start)[:, None] - jnp.arange(LANES)[None, :]
        stats = table_scores(ar, hid, ln, norm_final.reshape(1, dim), tgt, embed_table)
        res = combine(stats, 4 + layers)
        return from_row(res[0, :rows]), from_row(res[1, :rows]), outs[0].reshape(k_cache.shape), outs[1].reshape(v_cache.shape)

    return jax.shard_map(decode_local, mesh=mesh, in_specs=arg_specs, out_specs=result_specs, check_vma=False)
```
